512 devices in a mesh: seq: 32 (over y, x), head: 8 (over z), dp: 2 (over core).
Axes of the slice: x: 4, y: 8, z: 8, core: 2. Of those that a mesh axis runs over, the one named last changes fastest.
Arguments:
- queries: bfloat16 [32768, 4096], P(('dp', 'seq'), 'head'), parts along dimension 0, may hold values from -200 to 200
- keys: bfloat16 [32768, 1024], P(('dp', 'seq'), 'head'), parts along dimension 0, may hold values from -4 to 4
- values: bfloat16 [32768, 1024], P(('dp', 'seq'), 'head'), parts along dimension 0, may hold values from -15 to 15
- doc_ids: int32 [32768], P(('dp', 'seq')), parts along dimension 0, may hold values from 0 to 7, as said below
- block_lists: int32 [256, 16], P(('dp', 'seq')), parts along dimension 0, may hold values from 0 to 128, as said below
- w_out: bfloat16 [4096, 4096], P('head'), may hold values from -0.09375 to 0.09375
Outputs:
- mixed: bfloat16 [32768, 4096], P(('dp', 'seq'), 'head'), parts along dimension 0
The draws below stay inside these ranges and needn't reach their ends.
There are 2 independent parts, one for each index of `dp`. The reference program is written for one: setup_inputs(seed, part) draws one part's arguments, and reference() takes and returns one part's arrays. A program takes and returns all parts, laid end to end along the dimension named above; an argument that names none is the same for every part. Nothing has to cross between parts.
Inputs may be any that keep to these rules, and one draw needn't show every extreme that they name: `block_lists`: row i lists the blocks that query block i reads: 16 entries, each a block of the sequence or the null value 128; the non-null entries of a row are distinct and include i. Blocks k * 4 to k * 4 + 3 lie on index k of seq; over the rows of one index of seq together, at most one distinct block of each other index of seq is named (so each index of seq sends at most one of its blocks to each other index). `doc_ids`: never falling along the sequence.
All inputs are finite; a program needn't handle non-finite values.
Results may differ from the reference program's by a relative error of at most 0.013.
Values may be sent and summed in bfloat16 or wider, within the bound.
No kernel may reach another device: no remote copies, remote signals or barrier semaphores. Data moves between devices by JAX's collectives and lax.ppermute only.
A program may use at most 64 MiB of HBM per device.

```python
import math
import jax
import jax.numpy as jnp
from jax import lax

D = 4096
QUERY_HEADS = 32
KEY_VALUE_HEADS = 8
HEAD_SIZE = 128
BLOCK_TOKENS = 128
TOPK = 16
DOCS = 8
SEQUENCE_TOKENS = 16384
BPD = 4
BLOCK_TOTAL = 128
N_HEAD = 8


def draw_queries(key, part):
    base_index = 2.0 * jax.random.truncated_normal(jax.random.fold_in(key, 21), -4.0, 4.0, (SEQUENCE_TOKENS, QUERY_HEADS * HEAD_SIZE), jnp.float32)
    return base_index.astype(jnp.bfloat16)


def draw_keys(key, part):
    base_index = jax.random.truncated_normal(jax.random.fold_in(key, 22), -4.0, 4.0, (SEQUENCE_TOKENS, KEY_VALUE_HEADS * HEAD_SIZE), jnp.float32)
    return base_index.astype(jnp.bfloat16)


def draw_doc_ids(key, part):
    first_len = jax.random.randint(jax.random.fold_in(key, 41), (1,), SEQUENCE_TOKENS * 5 // 8, SEQUENCE_TOKENS * 3 // 4, dtype=jnp.int32)
    others = jax.random.randint(jax.random.fold_in(key, 42), (DOCS - 2,), 0, SEQUENCE_TOKENS, dtype=jnp.int32)
    others = first_len + 1 + others % (SEQUENCE_TOKENS - first_len - 1)
    bounds = jnp.concatenate([first_len, others]).astype(jnp.int32)
    positions = jnp.arange(SEQUENCE_TOKENS, dtype=jnp.int32)
    return jnp.sum((positions[:, None] >= bounds[None, :]).astype(jnp.int32), axis=1).astype(jnp.int32)


def draw_block_lists(key, part):
    seq_devices = BLOCK_TOTAL // BPD
    remote = min(TOPK - BPD, seq_devices - 1)
    padding = TOPK - BPD - remote
    offsets = jax.random.randint(jax.random.fold_in(key, 31), (seq_devices, seq_devices), 0, BPD, dtype=jnp.int32)
    owner_ids = jnp.arange(seq_devices, dtype=jnp.int32)

    def one_row(row):
        device = row // BPD
        shuffled = jax.random.permutation(jax.random.fold_in(jax.random.fold_in(key, 32), row), seq_devices).astype(jnp.int32)
        distance = jnp.abs(owner_ids - device)
        score = shuffled + 1 + jnp.where(distance <= 2, 4 * seq_devices, 0)
        score = score + jnp.where(owner_ids == (device + seq_devices // 2) % seq_devices, 2 * seq_devices, 0)
        score = jnp.where(owner_ids != device, score, 0)
        best, chosen = lax.top_k(score, remote)
        picked = jnp.where(best > 0, chosen * BPD + offsets[device, chosen], BLOCK_TOTAL).astype(jnp.int32)
        own_blocks = (device * BPD + jnp.arange(BPD, dtype=jnp.int32)).astype(jnp.int32)
        return jnp.concatenate([own_blocks, picked, jnp.full((padding,), BLOCK_TOTAL, jnp.int32)])
    return jax.vmap(one_row)(jnp.arange(BLOCK_TOTAL, dtype=jnp.int32))


def block_scale(key, shape, cuts, smallest, high):
    factor_of, own = 1.0, jax.random.fold_in(key, 6)
    for position, parts in cuts:
        heights = jnp.exp(jax.random.uniform(jax.random.fold_in(own, position), (parts,), jnp.float32, smallest / len(cuts), high / len(cuts)))
        factor_of = factor_of * jnp.repeat(heights, shape[position] // parts).reshape([-1 if axis == position else 1 for axis in range(len(shape))])
    return factor_of


def bell_draw(own_key, extent, scale, reach, shards=(), kind=jnp.bfloat16):
    array = scale * jax.random.normal(own_key, extent, jnp.float32)
    if shards:
        array = array * block_scale(own_key, extent, shards, -0.22, 0.18)
    return jnp.clip(array, -reach, reach).astype(kind)


def setup_inputs(seed: int = 0, part: int = 0) -> dict:
    splits = jax.random.split(jax.random.key(seed), 7)
    part_splits = jax.random.split(jax.random.fold_in(splits[6], part), 7)
    queries = draw_queries(jax.random.fold_in(jax.random.fold_in(splits[6], part), 71), part)
    keys = draw_keys(jax.random.fold_in(jax.random.fold_in(splits[6], part), 71), part)
    values = bell_draw(part_splits[2], (SEQUENCE_TOKENS, KEY_VALUE_HEADS * HEAD_SIZE), 3.0, 15.0, ((0, 32), (1, 8)))
    doc_ids = draw_doc_ids(jax.random.fold_in(jax.random.fold_in(splits[6], part), 71), part)
    block_lists = draw_block_lists(jax.random.fold_in(jax.random.fold_in(splits[6], part), 71), part)
    w_out = bell_draw(splits[5], (QUERY_HEADS * HEAD_SIZE, D), (QUERY_HEADS * HEAD_SIZE) ** -0.5, 0.09375, ((0, 8),))
    return {"queries": queries, "keys": keys, "values": values, "doc_ids": doc_ids, "block_lists": block_lists, "w_out": w_out}


negative = -1e+30
far_position = 1073741824

def block_terms(query_block, key_rows, value_rows, allowed):
    scores = jnp.einsum('qhge,jkhe->hgqjk', query_block.astype(jnp.float32), key_rows.astype(jnp.float32)) * (1.0 / math.sqrt(HEAD_SIZE))
    masked = jnp.where(allowed[None, None], scores, negative)
    block_top = lax.optimization_barrier(jnp.max(masked, axis=-1))
    probs = jnp.where(allowed[None, None], jnp.exp(masked - block_top[..., None]), 0.0)
    block_sum = lax.optimization_barrier(jnp.sum(probs, axis=-1))
    weights = probs.astype(jnp.bfloat16)
    partial_value = jnp.einsum('hgqjk,jkhe->hgqje', weights.astype(jnp.float32), value_rows.astype(jnp.float32))
    return (block_top, block_sum, partial_value)

def finish(block_top, block_sum, partial_value):
    row_peak = lax.optimization_barrier(jnp.max(block_top, axis=-1))
    factor = jnp.exp(block_top - row_peak[..., None])
    numer = lax.optimization_barrier(jnp.sum(factor[..., None] * partial_value, axis=3))
    denom = lax.optimization_barrier(jnp.sum(factor * block_sum, axis=-1))
    result = numer / denom[..., None]
    rows = result.shape[2]
    return jnp.transpose(result, (2, 0, 1, 3)).reshape(rows, -1).astype(jnp.bfloat16)

def reference(queries, keys, values, doc_ids, block_lists, w_out):
    group_count = QUERY_HEADS // KEY_VALUE_HEADS
    positions = jnp.arange(SEQUENCE_TOKENS, dtype=jnp.int32)
    doc_range = jnp.arange(DOCS, dtype=jnp.int32)
    doc_match = doc_ids[:, None] == doc_range[None, :]
    firsts = lax.optimization_barrier(jnp.min(jnp.where(doc_match, positions[:, None], far_position), axis=0)).astype(jnp.int32)
    later = doc_range[None, :] > doc_range[:, None]
    ends_doc = lax.optimization_barrier(jnp.min(jnp.where(later, firsts[None, :], far_position), axis=1)).astype(jnp.int32)
    starts = lax.optimization_barrier(jnp.sum(jnp.where(doc_match, firsts[None, :], 0), axis=1)).astype(jnp.int32)
    ends = lax.optimization_barrier(jnp.sum(jnp.where(doc_match, ends_doc[None, :], 0), axis=1)).astype(jnp.int32)
    empty_block = jnp.zeros((1, BLOCK_TOKENS, KEY_VALUE_HEADS, HEAD_SIZE), jnp.bfloat16)
    key_lookup = jnp.concatenate([keys.reshape(BLOCK_TOTAL, BLOCK_TOKENS, KEY_VALUE_HEADS, HEAD_SIZE), empty_block], axis=0)
    value_lookup = jnp.concatenate([values.reshape(BLOCK_TOTAL, BLOCK_TOKENS, KEY_VALUE_HEADS, HEAD_SIZE), empty_block], axis=0)
    query_tiles = queries.reshape(BLOCK_TOTAL, BLOCK_TOKENS, KEY_VALUE_HEADS, group_count, HEAD_SIZE)
    inside = jnp.arange(BLOCK_TOKENS, dtype=jnp.int32)

    def per_block(inputs):
        query_block, lists_row, query_start, query_end = inputs
        key_rows = jnp.take(key_lookup, lists_row, axis=0)
        value_rows = jnp.take(value_lookup, lists_row, axis=0)
        usable = lists_row < BLOCK_TOTAL
        key_pos = lists_row[:, None] * BLOCK_TOKENS + inside[None, :]
        allowed = usable[None, :, None] & (key_pos[None] < query_end[:, None, None]) & (key_pos[None] >= query_start[:, None, None])
        return finish(*block_terms(query_block, key_rows, value_rows, allowed))
    attn = lax.map(per_block, (query_tiles, block_lists, starts.reshape(BLOCK_TOTAL, BLOCK_TOKENS), ends.reshape(BLOCK_TOTAL, BLOCK_TOKENS)))
    attn = attn.reshape(SEQUENCE_TOKENS, QUERY_HEADS * HEAD_SIZE)
    cols = QUERY_HEADS * HEAD_SIZE // N_HEAD

    def add_group(running, group):
        attn_cols = lax.dynamic_slice_in_dim(attn, group * cols, cols, 1)
        weight_rows = lax.dynamic_slice_in_dim(w_out, group * cols, cols, 0)
        part = jnp.dot(attn_cols, weight_rows, preferred_element_type=jnp.float32).astype(jnp.bfloat16)
        part = lax.optimization_barrier(part)
        return (running + part.astype(jnp.float32), None)
    summed, _ = lax.scan(add_group, jnp.zeros((SEQUENCE_TOKENS, D), jnp.float32), jnp.arange(N_HEAD, dtype=jnp.int32))
    return summed.astype(jnp.bfloat16)
```

```python
import functools
import math

import jax
import jax.numpy as jnp
from jax import lax
from jax.experimental import pallas as pl
from jax.experimental.pallas import tpu as pltpu
from jax.sharding import Mesh, PartitionSpec as P

HEAD_SIZE = 128
BLOCK_TOKENS = 128
DOCS = 8
TOPK = 16
CHUNK = 4

negative = -1e30
far_position = 1073741824
null_base = -1073741824
score_scale = math.log2(math.e) / math.sqrt(HEAD_SIZE)


def attention_kernel(
    k_slot, v_slot, base, q_ref, start_ref, end_ref, *refs
):
    *pieces, out_ref, k_table, v_table, q4, kcat, vcat, scores = refs
    k_pieces, v_pieces = pieces[:-2], pieces[-2:]
    row = pl.program_id(0)
    heads = q_ref.shape[1] // HEAD_SIZE
    keys = CHUNK * BLOCK_TOKENS

    @pl.when(row == 0)
    def _():
        vcat[:, HEAD_SIZE:] = jnp.ones((vcat.shape[0], HEAD_SIZE), vcat.dtype)
        for table, pieces in ((k_table, k_pieces), (v_table, v_pieces)):
            at = 0
            for piece in pieces:
                table[at : at + piece.shape[0]] = piece[...]
                at += piece.shape[0]

    for h in range(heads):
        q4[h * BLOCK_TOKENS : (h + 1) * BLOCK_TOKENS, :] = q_ref[
            :, h * HEAD_SIZE : (h + 1) * HEAD_SIZE
        ]
    for j in range(TOPK):
        rows = slice(j * BLOCK_TOKENS, (j + 1) * BLOCK_TOKENS)
        kcat[rows, :] = k_table[k_slot[row * TOPK + j]]
        vcat[rows, :HEAD_SIZE] = v_table[v_slot[row * TOPK + j]]
    starts = start_ref[...]
    ends = end_ref[...]
    lane = lax.broadcasted_iota(jnp.int32, (BLOCK_TOKENS, BLOCK_TOKENS), 1)
    peak = None
    for c in range(TOPK // CHUNK):
        cols = slice(c * keys, (c + 1) * keys)
        bias = []
        for j in range(c * CHUNK, (c + 1) * CHUNK):
            position = lane + base[row * TOPK + j]
            allowed = (position >= starts) & (position < ends)
            bias.append(jnp.where(allowed, 0.0, negative))
        bias = jnp.concatenate(bias, axis=1)
        raw = lax.dot_general(
            q4[...], kcat[cols, :], (((1,), (1,)), ((), ())), preferred_element_type=jnp.float32
        )
        for h in range(heads):
            rows = slice(h * BLOCK_TOKENS, (h + 1) * BLOCK_TOKENS)
            scores[rows, cols] = raw[rows] * score_scale + bias
        part = scores[:, cols]
        for j in range(CHUNK):
            piece = part[:, j * BLOCK_TOKENS : (j + 1) * BLOCK_TOKENS]
            peak = piece if peak is None else jnp.maximum(peak, piece)
    top = jnp.max(peak, axis=1, keepdims=True)
    total = jnp.zeros((heads * BLOCK_TOKENS, 2 * HEAD_SIZE), jnp.float32)
    for c in range(TOPK // CHUNK):
        cols = slice(c * keys, (c + 1) * keys)
        weights = jnp.exp2(scores[:, cols] - top).astype(jnp.bfloat16)
        total += jnp.dot(weights, vcat[cols, :], preferred_element_type=jnp.float32)
    result = (total[:, :HEAD_SIZE] / total[:, HEAD_SIZE:]).astype(out_ref.dtype)
    for h in range(heads):
        out_ref[:, h * HEAD_SIZE : (h + 1) * HEAD_SIZE] = result[
            h * BLOCK_TOKENS : (h + 1) * BLOCK_TOKENS
        ]


def attention(queries, starts, ends, k_pieces, v_pieces, k_slot, v_slot, base):
    tokens, width = queries.shape
    blocks = tokens // BLOCK_TOKENS
    heads = width // HEAD_SIZE
    rows = heads * BLOCK_TOKENS
    listed = TOPK * BLOCK_TOKENS
    per_block = lambda i, *_: (i, 0)
    whole = lambda i, *_: (0, 0, 0)
    block = (BLOCK_TOKENS, HEAD_SIZE)
    return pl.pallas_call(
        attention_kernel,
        out_shape=jax.ShapeDtypeStruct((tokens, width), jnp.bfloat16),
        grid_spec=pltpu.PrefetchScalarGridSpec(
            num_scalar_prefetch=3,
            grid=(blocks,),
            in_specs=[
                pl.BlockSpec((BLOCK_TOKENS, width), per_block),
                pl.BlockSpec((BLOCK_TOKENS, BLOCK_TOKENS), per_block),
                pl.BlockSpec((BLOCK_TOKENS, BLOCK_TOKENS), per_block),
                *[pl.BlockSpec(piece.shape, whole) for piece in (*k_pieces, *v_pieces)],
            ],
            out_specs=pl.BlockSpec((BLOCK_TOKENS, width), per_block),
            scratch_shapes=[
                pltpu.VMEM((sum(p.shape[0] for p in k_pieces), *block), jnp.bfloat16),
                pltpu.VMEM((sum(p.shape[0] for p in v_pieces), *block), jnp.bfloat16),
                pltpu.VMEM((rows, HEAD_SIZE), jnp.bfloat16),
                pltpu.VMEM((listed, HEAD_SIZE), jnp.bfloat16),
                pltpu.VMEM((listed, 2 * HEAD_SIZE), jnp.bfloat16),
                pltpu.VMEM((rows, listed), jnp.float32),
            ],
        ),
        compiler_params=pltpu.CompilerParams(vmem_limit_bytes=32 * 1024 * 1024),
        cost_estimate=pl.CostEstimate(
            flops=4 * blocks * rows * listed * HEAD_SIZE,
            bytes_accessed=4 * 1024 * 1024,
            transcendentals=blocks * rows * listed,
        ),
        name="attention",
    )(k_slot, v_slot, base, queries, starts, ends, *k_pieces, *v_pieces)


def pick_kernel(index, source_ref, *out_refs):
    at = 0
    for out_ref in out_refs:
        for r in range(out_ref.shape[0]):
            out_ref[r] = source_ref[index[at]]
            at += 1


def pick(source, index, counts):
    return pl.pallas_call(
        pick_kernel,
        out_shape=[
            jax.ShapeDtypeStruct((count, *source.shape[1:]), source.dtype) for count in counts
        ],
        in_specs=[
            pl.BlockSpec(memory_space=pltpu.SMEM),
            pl.BlockSpec(memory_space=pltpu.VMEM),
        ],
        out_specs=[pl.BlockSpec(memory_space=pltpu.VMEM)] * len(counts),
        cost_estimate=pl.CostEstimate(
            flops=2 * 1024 * 1024, bytes_accessed=2 * 1024 * 1024, transcendentals=0
        ),
        name="pick",
    )(index, source)


def per_device(y_count, x_count, queries, keys, values, doc_ids, block_lists, w_out):
    tok_rows = queries.shape[0]
    blocks_dev = tok_rows // BLOCK_TOKENS
    seq_count = y_count * x_count
    block_count = blocks_dev * seq_count
    own_y, own_x = lax.axis_index("y"), lax.axis_index("x")
    own_index = own_y * x_count + own_x

    column_keys = lax.all_gather(keys, "y", axis=0, tiled=True)
    column_keys = column_keys.reshape(y_count * blocks_dev, BLOCK_TOKENS, HEAD_SIZE)

    positions = own_index * tok_rows + jnp.arange(tok_rows, dtype=jnp.int32)
    doc_range = jnp.arange(DOCS, dtype=jnp.int32)
    first_local = jnp.min(
        jnp.where(doc_ids[None, :] == doc_range[:, None], positions[None, :], far_position), axis=1
    )
    info = jnp.concatenate([block_lists.reshape(-1), first_local])
    info = lax.all_to_all(
        jnp.broadcast_to(info[None], (seq_count, info.shape[0])), ("y", "x"), 0, 0, tiled=True
    )
    entries = blocks_dev * TOPK
    listing = info[:, :entries]
    firsts = jnp.min(info[:, entries:], axis=0)

    owned = (listing < block_count) & (listing // blocks_dev == own_index)
    send_offset = jnp.max(jnp.where(owned, listing % blocks_dev, 0), axis=1)
    value_blocks = values.reshape(blocks_dev, BLOCK_TOKENS, HEAD_SIZE)
    (value_out,) = pick(value_blocks, send_offset, (seq_count,))
    value_in = lax.all_to_all(value_out, ("y", "x"), 0, 0, tiled=True)

    row_lists = lax.dynamic_slice_in_dim(listing, own_y * x_count, x_count, 0)
    shifts = jnp.arange(1, x_count, dtype=jnp.int32)
    readers = jnp.take(row_lists, (own_x + shifts) % x_count, axis=0)
    column = jnp.arange(y_count, dtype=jnp.int32)
    owners = column * x_count + own_x
    wanted = (readers[:, None, :] < block_count) & (
        readers[:, None, :] // blocks_dev == owners[None, :, None]
    )
    key_offset = jnp.max(jnp.where(wanted, readers[:, None, :] % blocks_dev, 0), axis=2)
    key_index = key_offset + (column * blocks_dev)[None, :]
    key_out = pick(column_keys, key_index.reshape(-1), (y_count,) * (x_count - 1))
    key_in = [
        lax.ppermute(piece, "x", [(i, (i + shift) % x_count) for i in range(x_count)])
        for shift, piece in enumerate(key_out, 1)
    ]

    valid = block_lists < block_count
    owner = block_lists // blocks_dev
    local = owner == own_index
    offset = block_lists % blocks_dev
    v_slot = jnp.where(valid, jnp.where(local, offset, blocks_dev + owner), 0).reshape(-1)
    owner_y, owner_x = owner // x_count, owner % x_count
    shift = (own_x - owner_x + x_count) % x_count
    far_slot = column_keys.shape[0] + (shift - 1) * y_count + owner_y
    k_slot = jnp.where(shift == 0, owner_y * blocks_dev + offset, far_slot)
    k_slot = jnp.where(valid, k_slot, 0).reshape(-1)
    base = jnp.where(valid, block_lists * BLOCK_TOKENS, null_base).reshape(-1)

    later = doc_range[None, :] > doc_range[:, None]
    ends_doc = jnp.min(jnp.where(later, firsts[None, :], far_position), axis=1)
    match = doc_ids[:, None] == doc_range[None, :]
    starts = jnp.sum(jnp.where(match, firsts[None, :], 0), axis=1)
    ends = jnp.sum(jnp.where(match, ends_doc[None, :], 0), axis=1)
    starts = jnp.broadcast_to(starts[:, None], (tok_rows, BLOCK_TOKENS))
    ends = jnp.broadcast_to(ends[:, None], (tok_rows, BLOCK_TOKENS))

    attn = attention(
        queries,
        starts,
        ends,
        (column_keys, *key_in),
        (value_blocks, value_in),
        k_slot,
        v_slot,
        base,
    )
    projected = jnp.dot(attn, w_out, preferred_element_type=jnp.float32).astype(jnp.bfloat16)
    return lax.psum_scatter(projected, "head", scatter_dimension=1, tiled=True)


def solution(mesh):
    seq_count = mesh.shape["seq"]
    x_count = 4 if seq_count % 4 == 0 else 1
    y_count = seq_count // x_count
    grid = Mesh(
        mesh.devices.reshape(y_count, x_count, mesh.shape["head"], mesh.shape["dp"]),
        ("y", "x", "head", "dp"),
    )
    rows = ("dp", "y", "x")
    in_specs = (
        P(rows, "head"),
        P(rows, "head"),
        P(rows, "head"),
        P(rows),
        P(rows, None),
        P("head", None),
    )
    return jax.shard_map(
        functools.partial(per_device, y_count, x_count),
        mesh=grid,
        in_specs=in_specs,
        out_specs=P(rows, "head"),
        check_vma=False,
    )
```

```python
import functools
import math

import jax
import jax.numpy as jnp
from jax import lax
from jax.experimental import pallas as pl
from jax.experimental.pallas import tpu as pltpu
from jax.sharding import Mesh, PartitionSpec as P

HEAD_SIZE = 128
BLOCK_TOKENS = 128
DOCS = 8
TOPK = 16
CHUNK = 4

negative = -1e30
far_position = 1073741824
null_base = -1073741824
score_scale = math.log2(math.e) / math.sqrt(HEAD_SIZE)


def attention_kernel(
    k_slot, v_slot, base, q_ref, start_ref, end_ref, w_ref, *refs
):
    *pieces, out_ref, k_table, v_table, q4, kcat, vcat, scores, attn = refs
    k_pieces, v_pieces = pieces[:-2], pieces[-2:]
    row = pl.program_id(0)
    heads = q_ref.shape[1] // HEAD_SIZE
    keys = CHUNK * BLOCK_TOKENS

    @pl.when(row == 0)
    def _():
        vcat[:, HEAD_SIZE:] = jnp.ones((vcat.shape[0], HEAD_SIZE), vcat.dtype)
        for table, pieces in ((k_table, k_pieces), (v_table, v_pieces)):
            at = 0
            for piece in pieces:
                table[at : at + piece.shape[0]] = piece[...]
                at += piece.shape[0]

    for h in range(heads):
        q4[h * BLOCK_TOKENS : (h + 1) * BLOCK_TOKENS, :] = q_ref[
            :, h * HEAD_SIZE : (h + 1) * HEAD_SIZE
        ]
    for j in range(TOPK):
        rows = slice(j * BLOCK_TOKENS, (j + 1) * BLOCK_TOKENS)
        kcat[rows, :] = k_table[k_slot[row * TOPK + j]]
        vcat[rows, :HEAD_SIZE] = v_table[v_slot[row * TOPK + j]]
    starts = start_ref[...]
    ends = end_ref[...]
    lane = lax.broadcasted_iota(jnp.int32, (BLOCK_TOKENS, BLOCK_TOKENS), 1)
    peak = None
    for c in range(TOPK // CHUNK):
        cols = slice(c * keys, (c + 1) * keys)
        bias = []
        for j in range(c * CHUNK, (c + 1) * CHUNK):
            position = lane + base[row * TOPK + j]
            allowed = (position >= starts) & (position < ends)
            bias.append(jnp.where(allowed, 0.0, negative))
        bias = jnp.concatenate(bias, axis=1)
        raw = lax.dot_general(
            q4[...], kcat[cols, :], (((1,), (1,)), ((), ())), preferred_element_type=jnp.float32
        )
        for h in range(heads):
            rows = slice(h * BLOCK_TOKENS, (h + 1) * BLOCK_TOKENS)
            scores[rows, cols] = raw[rows] * score_scale + bias
        part = scores[:, cols]
        for j in range(CHUNK):
            piece = part[:, j * BLOCK_TOKENS : (j + 1) * BLOCK_TOKENS]
            peak = piece if peak is None else jnp.maximum(peak, piece)
    top = jnp.max(peak, axis=1, keepdims=True)
    total = jnp.zeros((heads * BLOCK_TOKENS, 2 * HEAD_SIZE), jnp.float32)
    for c in range(TOPK // CHUNK):
        cols = slice(c * keys, (c + 1) * keys)
        weights = jnp.exp2(scores[:, cols] - top).astype(jnp.bfloat16)
        total += jnp.dot(weights, vcat[cols, :], preferred_element_type=jnp.float32)
    result = (total[:, :HEAD_SIZE] / total[:, HEAD_SIZE:]).astype(attn.dtype)
    for h in range(heads):
        attn[:, h * HEAD_SIZE : (h + 1) * HEAD_SIZE] = result[
            h * BLOCK_TOKENS : (h + 1) * BLOCK_TOKENS
        ]
    step = 1024
    for c in range(0, w_ref.shape[1], step):
        out_ref[:, c : c + step] = jnp.dot(
            attn[...], w_ref[:, c : c + step], preferred_element_type=jnp.float32
        ).astype(out_ref.dtype)


def attention(queries, starts, ends, w_out, k_pieces, v_pieces, k_slot, v_slot, base):
    tokens, width = queries.shape
    blocks = tokens // BLOCK_TOKENS
    heads = width // HEAD_SIZE
    rows = heads * BLOCK_TOKENS
    listed = TOPK * BLOCK_TOKENS
    per_block = lambda i, *_: (i, 0)
    whole = lambda i, *_: (0, 0, 0)
    block = (BLOCK_TOKENS, HEAD_SIZE)
    return pl.pallas_call(
        attention_kernel,
        out_shape=jax.ShapeDtypeStruct((tokens, w_out.shape[1]), jnp.bfloat16),
        grid_spec=pltpu.PrefetchScalarGridSpec(
            num_scalar_prefetch=3,
            grid=(blocks,),
            in_specs=[
                pl.BlockSpec((BLOCK_TOKENS, width), per_block),
                pl.BlockSpec((BLOCK_TOKENS, BLOCK_TOKENS), per_block),
                pl.BlockSpec((BLOCK_TOKENS, BLOCK_TOKENS), per_block),
                pl.BlockSpec(w_out.shape, lambda i, *_: (0, 0)),
                *[pl.BlockSpec(piece.shape, whole) for piece in (*k_pieces, *v_pieces)],
            ],
            out_specs=pl.BlockSpec((BLOCK_TOKENS, w_out.shape[1]), per_block),
            scratch_shapes=[
                pltpu.VMEM((sum(p.shape[0] for p in k_pieces), *block), jnp.bfloat16),
                pltpu.VMEM((sum(p.shape[0] for p in v_pieces), *block), jnp.bfloat16),
                pltpu.VMEM((rows, HEAD_SIZE), jnp.bfloat16),
                pltpu.VMEM((listed, HEAD_SIZE), jnp.bfloat16),
                pltpu.VMEM((listed, 2 * HEAD_SIZE), jnp.bfloat16),
                pltpu.VMEM((rows, listed), jnp.float32),
                pltpu.VMEM((BLOCK_TOKENS, width), jnp.bfloat16),
            ],
        ),
        compiler_params=pltpu.CompilerParams(vmem_limit_bytes=32 * 1024 * 1024),
        cost_estimate=pl.CostEstimate(
            flops=4 * blocks * rows * listed * HEAD_SIZE + 2 * tokens * width * w_out.shape[1],
            bytes_accessed=4 * 1024 * 1024,
            transcendentals=blocks * rows * listed,
        ),
        name="attention",
    )(k_slot, v_slot, base, queries, starts, ends, w_out, *k_pieces, *v_pieces)


def pick_kernel(index, source_ref, out_ref):
    for r in range(out_ref.shape[0]):
        out_ref[r] = source_ref[index[r]]


def pick_column_kernel(piece_count, index, *refs):
    pieces, out_refs = refs[:piece_count], refs[piece_count:]
    for s, out_ref in enumerate(out_refs):
        for d, piece in enumerate(pieces):
            out_ref[d] = piece[index[s * piece_count + d]]


def small_kernel(body, out_shape, name, scalars, *operands):
    return pl.pallas_call(
        body,
        out_shape=out_shape,
        in_specs=[pl.BlockSpec(memory_space=pltpu.SMEM)]
        + [pl.BlockSpec(memory_space=pltpu.VMEM)] * len(operands),
        out_specs=jax.tree.map(lambda _: pl.BlockSpec(memory_space=pltpu.VMEM), out_shape),
        compiler_params=pltpu.CompilerParams(vmem_limit_bytes=8 * 1024 * 1024),
        cost_estimate=pl.CostEstimate(
            flops=1024 * 1024, bytes_accessed=1024 * 1024, transcendentals=0
        ),
        name=name,
    )(scalars, *operands)


def pick(source, index):
    out = jax.ShapeDtypeStruct((index.shape[0], *source.shape[1:]), source.dtype)
    return small_kernel(pick_kernel, out, "pick", index, source)


def pick_column(pieces, index, count):
    out = [
        jax.ShapeDtypeStruct((len(pieces), *pieces[0].shape[1:]), pieces[0].dtype)
    ] * count
    body = functools.partial(pick_column_kernel, len(pieces))
    return small_kernel(body, out, "pick_column", index, *pieces)


def shifted(x, axis, shift):
    size = lax.axis_size(axis)
    return lax.ppermute(x, axis, [(i, (i + shift) % size) for i in range(size)])


def ring_gather(x, axis):
    size = lax.axis_size(axis)
    pieces = {0: x}
    for step in range(1, size // 2 + 1):
        pieces[step] = shifted(pieces[step - 1], axis, 1)
        if size - step > step:
            pieces[size - step] = shifted(pieces[(size - step + 1) % size], axis, -1)
    return [pieces[d] for d in range(size)]


def add_kernel(size, groups, me, partial_ref, *refs):
    out_ref = refs[-1]
    arrived = list(refs[:-1])
    at = 0
    for first, rows, distance, terms in groups:
        width = out_ref.shape[1]
        column = pl.multiple_of(lax.rem(me[0] + (distance + size), size) * width, width)
        total = partial_ref[first : first + rows, pl.ds(column, width)].astype(jnp.float32)
        for _ in range(terms):
            total += arrived.pop(0)[...].astype(jnp.float32)
        out_ref[at : at + rows, :] = total.astype(out_ref.dtype)
        at += rows


def ring_scatter(partial, axis, streams):
    size = lax.axis_size(axis)
    me = lax.axis_index(axis).reshape(1).astype(jnp.int32)
    width = partial.shape[1] // size
    rows = partial.shape[0] // streams

    def add(groups, *arrived):
        out = jax.ShapeDtypeStruct((sum(g[1] for g in groups), width), partial.dtype)
        body = functools.partial(add_kernel, size, groups)
        return small_kernel(body, out, "ring_add", me, partial, *arrived)

    far = size // 2
    lengths = [(far, size - 1 - far) if b % 2 == 0 else (size - 1 - far, far) for b in range(streams)]
    sums = [[None, None] for _ in range(streams)]
    for b in range(streams):
        for side, sign in enumerate((1, -1)):
            sums[b][side] = add(((b * rows, rows, sign * lengths[b][side], 0),))
    for step in range(1, far + 1):
        for b in range(streams):
            for side, sign in enumerate((1, -1)):
                left = lengths[b][side] - step
                if left < 0:
                    continue
                moved = shifted(sums[b][side], axis, sign)
                if left:
                    moved = add(((b * rows, rows, sign * left, 1),), moved)
                sums[b][side] = moved
    groups = tuple((b * rows, rows, 0, 2) for b in range(streams))
    return add(groups, *[term for pair in sums for term in pair])


def per_device(y_count, x_count, queries, keys, values, doc_ids, block_lists, w_out):
    tok_rows = queries.shape[0]
    blocks_dev = tok_rows // BLOCK_TOKENS
    seq_count = y_count * x_count
    block_count = blocks_dev * seq_count
    own_y, own_x = lax.axis_index("y"), lax.axis_index("x")
    own_index = own_y * x_count + own_x

    key_blocks = keys.reshape(blocks_dev, BLOCK_TOKENS, HEAD_SIZE)
    value_blocks = values.reshape(blocks_dev, BLOCK_TOKENS, HEAD_SIZE)
    column_keys = ring_gather(key_blocks, "y")

    positions = own_index * tok_rows + jnp.arange(tok_rows, dtype=jnp.int32)
    doc_range = jnp.arange(DOCS, dtype=jnp.int32)
    first_local = jnp.min(
        jnp.where(doc_ids[None, :] == doc_range[:, None], positions[None, :], far_position), axis=1
    )
    info = jnp.concatenate([block_lists.reshape(-1), first_local])
    info = lax.all_to_all(
        jnp.broadcast_to(info[None], (seq_count, info.shape[0])), ("y", "x"), 0, 0, tiled=True
    )
    entries = blocks_dev * TOPK
    listing = info[:, :entries]
    firsts = jnp.min(info[:, entries:], axis=0)

    owned = (listing < block_count) & (listing // blocks_dev == own_index)
    send_offset = jnp.max(jnp.where(owned, listing % blocks_dev, 0), axis=1)
    value_out = pick(value_blocks, send_offset)
    value_in = lax.all_to_all(value_out, ("y", "x"), 0, 0, tiled=True)

    row_lists = lax.dynamic_slice_in_dim(listing, own_y * x_count, x_count, 0)
    shifts = jnp.arange(1, x_count, dtype=jnp.int32)
    readers = jnp.take(row_lists, (own_x + shifts) % x_count, axis=0)
    back = jnp.arange(y_count, dtype=jnp.int32)
    owners = (own_y - back + y_count) % y_count * x_count + own_x
    wanted = (readers[:, None, :] < block_count) & (
        readers[:, None, :] // blocks_dev == owners[None, :, None]
    )
    key_offset = jnp.max(jnp.where(wanted, readers[:, None, :] % blocks_dev, 0), axis=2)
    key_out = pick_column(column_keys, key_offset.reshape(-1), x_count - 1)
    key_in = [shifted(piece, "x", shift) for shift, piece in enumerate(key_out, 1)]

    valid = block_lists < block_count
    owner = block_lists // blocks_dev
    local = owner == own_index
    offset = block_lists % blocks_dev
    v_slot = jnp.where(valid, jnp.where(local, offset, blocks_dev + owner), 0).reshape(-1)
    owner_y, owner_x = owner // x_count, owner % x_count
    shift = (own_x - owner_x + x_count) % x_count
    back = (own_y - owner_y + y_count) % y_count
    far_slot = y_count * blocks_dev + (shift - 1) * y_count + back
    k_slot = jnp.where(shift == 0, back * blocks_dev + offset, far_slot)
    k_slot = jnp.where(valid, k_slot, 0).reshape(-1)
    base = jnp.where(valid, block_lists * BLOCK_TOKENS, null_base).reshape(-1)

    later = doc_range[None, :] > doc_range[:, None]
    ends_doc = jnp.min(jnp.where(later, firsts[None, :], far_position), axis=1)
    match = doc_ids[:, None] == doc_range[None, :]
    starts = jnp.sum(jnp.where(match, firsts[None, :], 0), axis=1)
    ends = jnp.sum(jnp.where(match, ends_doc[None, :], 0), axis=1)
    starts = jnp.broadcast_to(starts[:, None], (tok_rows, BLOCK_TOKENS))
    ends = jnp.broadcast_to(ends[:, None], (tok_rows, BLOCK_TOKENS))

    partial = attention(
        queries,
        starts,
        ends,
        w_out,
        (*column_keys, *key_in),
        (value_blocks, value_in),
        k_slot,
        v_slot,
        base,
    )
    return ring_scatter(partial, "head", 2)


def solution(mesh):
    seq_count = mesh.shape["seq"]
    x_count = 4 if seq_count % 4 == 0 else 1
    y_count = seq_count // x_count
    grid = Mesh(
        mesh.devices.reshape(y_count, x_count, mesh.shape["head"], mesh.shape["dp"]),
        ("y", "x", "head", "dp"),
    )
    rows = ("dp", "y", "x")
    in_specs = (
        P(rows, "head"),
        P(rows, "head"),
        P(rows, "head"),
        P(rows),
        P(rows, None),
        P("head", None),
    )
    return jax.shard_map(
        functools.partial(per_device, y_count, x_count),
        mesh=grid,
        in_specs=in_specs,
        out_specs=P(rows, "head"),
        check_vma=False,
    )
```

```python
import functools
import math

import jax
import jax.numpy as jnp
from jax import lax
from jax.experimental import pallas as pl
from jax.experimental.pallas import tpu as pltpu
from jax.sharding import Mesh, PartitionSpec as P

HEAD_SIZE = 128
BLOCK_TOKENS = 128
DOCS = 8
TOPK = 16
CHUNK = 4

negative = -1e30
far_position = 1073741824
null_base = -1073741824
score_scale = math.log2(math.e) / math.sqrt(HEAD_SIZE)


def weights_kernel(k_slot, base, q_ref, start_ref, end_ref, *refs):
    *pieces, out_ref, table, q4, kcat, scores = refs
    row = pl.program_id(0)
    heads = q_ref.shape[1] // HEAD_SIZE
    keys = CHUNK * BLOCK_TOKENS

    @pl.when(row == 0)
    def _():
        at = 0
        for piece in pieces:
            table[at : at + piece.shape[0]] = piece[...]
            at += piece.shape[0]

    for h in range(heads):
        q4[h * BLOCK_TOKENS : (h + 1) * BLOCK_TOKENS, :] = q_ref[
            :, h * HEAD_SIZE : (h + 1) * HEAD_SIZE
        ]
    for j in range(TOPK):
        kcat[j * BLOCK_TOKENS : (j + 1) * BLOCK_TOKENS, :] = table[k_slot[row * TOPK + j]]
    starts = start_ref[...]
    ends = end_ref[...]
    lane = lax.broadcasted_iota(jnp.int32, (BLOCK_TOKENS, BLOCK_TOKENS), 1)
    peak = None
    for c in range(TOPK // CHUNK):
        cols = slice(c * keys, (c + 1) * keys)
        bias = []
        for j in range(c * CHUNK, (c + 1) * CHUNK):
            position = lane + base[row * TOPK + j]
            allowed = (position >= starts) & (position < ends)
            bias.append(jnp.where(allowed, 0.0, negative))
        bias = jnp.concatenate(bias, axis=1)
        raw = lax.dot_general(
            q4[...], kcat[cols, :], (((1,), (1,)), ((), ())), preferred_element_type=jnp.float32
        )
        for h in range(heads):
            rows = slice(h * BLOCK_TOKENS, (h + 1) * BLOCK_TOKENS)
            scores[rows, cols] = raw[rows] * score_scale + bias
        part = scores[:, cols]
        for j in range(CHUNK):
            piece = part[:, j * BLOCK_TOKENS : (j + 1) * BLOCK_TOKENS]
            peak = piece if peak is None else jnp.maximum(peak, piece)
    top = jnp.max(peak, axis=1, keepdims=True)
    for c in range(TOPK // CHUNK):
        cols = slice(c * keys, (c + 1) * keys)
        out_ref[:, cols] = jnp.exp2(scores[:, cols] - top).astype(out_ref.dtype)


def weights_of(queries, starts, ends, pieces, k_slot, base):
    tokens, width = queries.shape
    blocks = tokens // BLOCK_TOKENS
    rows = width // HEAD_SIZE * BLOCK_TOKENS
    listed = TOPK * BLOCK_TOKENS
    per_block = lambda i, *_: (i, 0)
    whole = lambda i, *_: (0, 0, 0)
    block = (BLOCK_TOKENS, HEAD_SIZE)
    return pl.pallas_call(
        weights_kernel,
        out_shape=jax.ShapeDtypeStruct((blocks * rows, listed), jnp.bfloat16),
        grid_spec=pltpu.PrefetchScalarGridSpec(
            num_scalar_prefetch=2,
            grid=(blocks,),
            in_specs=[
                pl.BlockSpec((BLOCK_TOKENS, width), per_block),
                pl.BlockSpec((BLOCK_TOKENS, BLOCK_TOKENS), per_block),
                pl.BlockSpec((BLOCK_TOKENS, BLOCK_TOKENS), per_block),
                *[pl.BlockSpec(piece.shape, whole) for piece in pieces],
            ],
            out_specs=pl.BlockSpec((rows, listed), per_block),
            scratch_shapes=[
                pltpu.VMEM((sum(p.shape[0] for p in pieces), *block), jnp.bfloat16),
                pltpu.VMEM((rows, HEAD_SIZE), jnp.bfloat16),
                pltpu.VMEM((listed, HEAD_SIZE), jnp.bfloat16),
                pltpu.VMEM((rows, listed), jnp.float32),
            ],
        ),
        compiler_params=pltpu.CompilerParams(vmem_limit_bytes=56 * 1024 * 1024),
        cost_estimate=pl.CostEstimate(
            flops=2 * blocks * rows * listed * HEAD_SIZE,
            bytes_accessed=4 * 1024 * 1024,
            transcendentals=blocks * rows * listed,
        ),
        name="weights",
    )(k_slot, base, queries, starts, ends, *pieces)


def project_kernel(v_slot, weights_ref, w_hbm, *refs):
    *pieces, out_ref, table, vcat, attn, w_ref, w_sem = refs
    row = pl.program_id(0)
    heads = attn.shape[1] // HEAD_SIZE
    keys = CHUNK * BLOCK_TOKENS
    w_copy = pltpu.make_async_copy(w_hbm, w_ref, w_sem)

    @pl.when(row == 0)
    def _():
        w_copy.start()
        vcat[:, HEAD_SIZE:] = jnp.ones((vcat.shape[0], HEAD_SIZE), vcat.dtype)
        at = 0
        for piece in pieces:
            table[at : at + piece.shape[0]] = piece[...]
            at += piece.shape[0]

    for j in range(TOPK):
        rows = slice(j * BLOCK_TOKENS, (j + 1) * BLOCK_TOKENS)
        vcat[rows, :HEAD_SIZE] = table[v_slot[row * TOPK + j]]
    total = jnp.zeros((heads * BLOCK_TOKENS, 2 * HEAD_SIZE), jnp.float32)
    for c in range(TOPK // CHUNK):
        cols = slice(c * keys, (c + 1) * keys)
        total += jnp.dot(weights_ref[:, cols], vcat[cols, :], preferred_element_type=jnp.float32)
    result = (total[:, :HEAD_SIZE] / total[:, HEAD_SIZE:]).astype(attn.dtype)
    for h in range(heads):
        attn[:, h * HEAD_SIZE : (h + 1) * HEAD_SIZE] = result[
            h * BLOCK_TOKENS : (h + 1) * BLOCK_TOKENS
        ]

    @pl.when(row == 0)
    def _():
        w_copy.wait()

    step = 1024
    for c in range(0, w_ref.shape[1], step):
        out_ref[:, c : c + step] = jnp.dot(
            attn[...], w_ref[:, c : c + step], preferred_element_type=jnp.float32
        ).astype(out_ref.dtype)


def project(weights, pieces, w_out, v_slot):
    width = w_out.shape[0]
    rows = width // HEAD_SIZE * BLOCK_TOKENS
    blocks = weights.shape[0] // rows
    tokens = blocks * BLOCK_TOKENS
    listed = weights.shape[1]
    per_block = lambda i, *_: (i, 0)
    whole = lambda i, *_: (0, 0, 0)
    block = (BLOCK_TOKENS, HEAD_SIZE)
    return pl.pallas_call(
        project_kernel,
        out_shape=jax.ShapeDtypeStruct((tokens, w_out.shape[1]), jnp.bfloat16),
        grid_spec=pltpu.PrefetchScalarGridSpec(
            num_scalar_prefetch=1,
            grid=(blocks,),
            in_specs=[
                pl.BlockSpec((rows, listed), per_block),
                pl.BlockSpec(memory_space=pl.ANY),
                *[pl.BlockSpec(piece.shape, whole) for piece in pieces],
            ],
            out_specs=pl.BlockSpec((BLOCK_TOKENS, w_out.shape[1]), per_block),
            scratch_shapes=[
                pltpu.VMEM((sum(p.shape[0] for p in pieces), *block), jnp.bfloat16),
                pltpu.VMEM((listed, 2 * HEAD_SIZE), jnp.bfloat16),
                pltpu.VMEM((BLOCK_TOKENS, width), jnp.bfloat16),
                pltpu.VMEM(w_out.shape, w_out.dtype),
                pltpu.SemaphoreType.DMA,
            ],
        ),
        compiler_params=pltpu.CompilerParams(vmem_limit_bytes=48 * 1024 * 1024),
        cost_estimate=pl.CostEstimate(
            flops=2 * blocks * rows * listed * HEAD_SIZE + 2 * tokens * width * w_out.shape[1],
            bytes_accessed=8 * 1024 * 1024,
            transcendentals=0,
        ),
        name="project",
    )(v_slot, weights, w_out, *pieces)


def pick_kernel(index, source_ref, *refs):
    out_ref = refs[-1]
    for r in range(out_ref.shape[0]):
        out_ref[r] = source_ref[index[r]]


def pick_column_kernel(piece_count, index, *refs):
    pieces, out_refs = refs[:piece_count], refs[piece_count:]
    for s, out_ref in enumerate(out_refs):
        for d, piece in enumerate(pieces):
            out_ref[d] = piece[index[s * piece_count + d]]


def small_kernel(body, out_shape, name, scalars, *operands):
    return pl.pallas_call(
        body,
        out_shape=out_shape,
        in_specs=[pl.BlockSpec(memory_space=pltpu.SMEM)]
        + [pl.BlockSpec(memory_space=pltpu.VMEM)] * len(operands),
        out_specs=jax.tree.map(lambda _: pl.BlockSpec(memory_space=pltpu.VMEM), out_shape),
        compiler_params=pltpu.CompilerParams(vmem_limit_bytes=8 * 1024 * 1024),
        cost_estimate=pl.CostEstimate(
            flops=1024 * 1024, bytes_accessed=1024 * 1024, transcendentals=0
        ),
        name=name,
    )(scalars, *operands)


def pick(source, index, *after):
    out = jax.ShapeDtypeStruct((index.shape[0], *source.shape[1:]), source.dtype)
    return small_kernel(pick_kernel, out, "pick", index, source, *after)


def pick_column(pieces, index, count):
    out = [
        jax.ShapeDtypeStruct((len(pieces), *pieces[0].shape[1:]), pieces[0].dtype)
    ] * count
    body = functools.partial(pick_column_kernel, len(pieces))
    return small_kernel(body, out, "pick_column", index, *pieces)


def shifted(x, axis, shift):
    size = lax.axis_size(axis)
    return lax.ppermute(x, axis, [(i, (i + shift) % size) for i in range(size)])


def ring_gather(x, axis):
    size = lax.axis_size(axis)
    pieces = {0: x}
    for step in range(1, size // 2 + 1):
        pieces[step] = shifted(pieces[step - 1], axis, 1)
        if size - step > step:
            pieces[size - step] = shifted(pieces[(size - step + 1) % size], axis, -1)
    return [pieces[d] for d in range(size)]


def add_kernel(size, groups, me, partial_ref, *refs):
    out_ref = refs[-1]
    arrived = list(refs[:-1])
    at = 0
    for first, rows, distance, terms in groups:
        width = out_ref.shape[1]
        column = pl.multiple_of(lax.rem(me[0] + (distance + size), size) * width, width)
        total = partial_ref[first : first + rows, pl.ds(column, width)].astype(jnp.float32)
        for _ in range(terms):
            total += arrived.pop(0)[...].astype(jnp.float32)
        out_ref[at : at + rows, :] = total.astype(out_ref.dtype)
        at += rows


def ring_scatter(partial, axis, streams):
    size = lax.axis_size(axis)
    me = lax.axis_index(axis).reshape(1).astype(jnp.int32)
    width = partial.shape[1] // size
    rows = partial.shape[0] // streams

    def add(groups, *arrived):
        out = jax.ShapeDtypeStruct((sum(g[1] for g in groups), width), partial.dtype)
        body = functools.partial(add_kernel, size, groups)
        return small_kernel(body, out, "ring_add", me, partial, *arrived)

    far = size // 2
    lengths = [(far, size - 1 - far) if b % 2 == 0 else (size - 1 - far, far) for b in range(streams)]
    sums = [[None, None] for _ in range(streams)]
    for b in range(streams):
        for side, sign in enumerate((1, -1)):
            sums[b][side] = add(((b * rows, rows, sign * lengths[b][side], 0),))
    for step in range(1, far + 1):
        for b in range(streams):
            for side, sign in enumerate((1, -1)):
                left = lengths[b][side] - step
                if left < 0:
                    continue
                moved = shifted(sums[b][side], axis, sign)
                if left:
                    moved = add(((b * rows, rows, sign * left, 1),), moved)
                sums[b][side] = moved
    groups = tuple((b * rows, rows, 0, 2) for b in range(streams))
    return add(groups, *[term for pair in sums for term in pair])


def per_device(y_count, x_count, queries, keys, values, doc_ids, block_lists, w_out):
    tok_rows = queries.shape[0]
    blocks_dev = tok_rows // BLOCK_TOKENS
    seq_count = y_count * x_count
    block_count = blocks_dev * seq_count
    own_y, own_x = lax.axis_index("y"), lax.axis_index("x")
    own_index = own_y * x_count + own_x

    key_blocks = keys.reshape(blocks_dev, BLOCK_TOKENS, HEAD_SIZE)
    value_blocks = values.reshape(blocks_dev, BLOCK_TOKENS, HEAD_SIZE)
    column_keys = ring_gather(key_blocks, "y")

    positions = own_index * tok_rows + jnp.arange(tok_rows, dtype=jnp.int32)
    doc_range = jnp.arange(DOCS, dtype=jnp.int32)
    first_local = jnp.min(
        jnp.where(doc_ids[None, :] == doc_range[:, None], positions[None, :], far_position), axis=1
    )
    info = jnp.concatenate([block_lists.reshape(-1), first_local])
    info = lax.all_to_all(
        jnp.broadcast_to(info[None], (seq_count, info.shape[0])), ("y", "x"), 0, 0, tiled=True
    )
    entries = blocks_dev * TOPK
    listing = info[:, :entries]
    firsts = jnp.min(info[:, entries:], axis=0)

    owned = (listing < block_count) & (listing // blocks_dev == own_index)
    send_offset = jnp.max(jnp.where(owned, listing % blocks_dev, 0), axis=1)
    half = y_count // 2
    value_out = pick(value_blocks, send_offset, column_keys[half], column_keys[half + 1])
    value_in = lax.all_to_all(value_out, ("y", "x"), 0, 0, tiled=True)

    row_lists = lax.dynamic_slice_in_dim(listing, own_y * x_count, x_count, 0)
    shifts = jnp.arange(1, x_count, dtype=jnp.int32)
    readers = jnp.take(row_lists, (own_x + shifts) % x_count, axis=0)
    back = jnp.arange(y_count, dtype=jnp.int32)
    owners = (own_y - back + y_count) % y_count * x_count + own_x
    wanted = (readers[:, None, :] < block_count) & (
        readers[:, None, :] // blocks_dev == owners[None, :, None]
    )
    key_offset = jnp.max(jnp.where(wanted, readers[:, None, :] % blocks_dev, 0), axis=2)
    key_out = pick_column(column_keys, key_offset.reshape(-1), x_count - 1)
    key_in = [shifted(piece, "x", shift) for shift, piece in enumerate(key_out, 1)]

    valid = block_lists < block_count
    owner = block_lists // blocks_dev
    local = owner == own_index
    offset = block_lists % blocks_dev
    v_slot = jnp.where(valid, jnp.where(local, offset, blocks_dev + owner), 0).reshape(-1)
    owner_y, owner_x = owner // x_count, owner % x_count
    shift = (own_x - owner_x + x_count) % x_count
    back = (own_y - owner_y + y_count) % y_count
    far_slot = y_count * blocks_dev + (shift - 1) * y_count + back
    k_slot = jnp.where(shift == 0, back * blocks_dev + offset, far_slot)
    k_slot = jnp.where(valid, k_slot, 0).reshape(-1)
    base = jnp.where(valid, block_lists * BLOCK_TOKENS, null_base).reshape(-1)

    later = doc_range[None, :] > doc_range[:, None]
    ends_doc = jnp.min(jnp.where(later, firsts[None, :], far_position), axis=1)
    match = doc_ids[:, None] == doc_range[None, :]
    starts = jnp.sum(jnp.where(match, firsts[None, :], 0), axis=1)
    ends = jnp.sum(jnp.where(match, ends_doc[None, :], 0), axis=1)
    starts = jnp.broadcast_to(starts[:, None], (tok_rows, BLOCK_TOKENS))
    ends = jnp.broadcast_to(ends[:, None], (tok_rows, BLOCK_TOKENS))

    weights = weights_of(queries, starts, ends, (*column_keys, *key_in), k_slot, base)
    partial = project(weights, (value_blocks, value_in), w_out, v_slot)
    return ring_scatter(partial, "head", 2)


def solution(mesh):
    seq_count = mesh.shape["seq"]
    x_count = 4 if seq_count % 4 == 0 else 1
    y_count = seq_count // x_count
    grid = Mesh(
        mesh.devices.reshape(y_count, x_count, mesh.shape["head"], mesh.shape["dp"]),
        ("y", "x", "head", "dp"),
    )
    rows = ("dp", "y", "x")
    in_specs = (
        P(rows, "head"),
        P(rows, "head"),
        P(rows, "head"),
        P(rows),
        P(rows, None),
        P("head", None),
    )
    return jax.shard_map(
        functools.partial(per_device, y_count, x_count),
        mesh=grid,
        in_specs=in_specs,
        out_specs=P(rows, "head"),
        check_vma=False,
    )
```

```python
import functools
import math

import jax
import jax.numpy as jnp
from jax import lax
from jax.experimental import pallas as pl
from jax.experimental.pallas import tpu as pltpu
from jax.sharding import Mesh, PartitionSpec as P

HEAD_SIZE = 128
BLOCK_TOKENS = 128
DOCS = 8
TOPK = 16
CHUNK = 4

negative = -1e30
far_position = 1073741824
null_base = -1073741824
score_scale = math.log2(math.e) / math.sqrt(HEAD_SIZE)


def attention_kernel(slot, base, q_ref, start_ref, end_ref, w_hbm, *refs):
    *pieces, out_ref, table, q4, kcat, vcat, scores, attn, w_ref, w_sem = refs
    row = pl.program_id(0)
    heads = q_ref.shape[1] // HEAD_SIZE
    keys = CHUNK * BLOCK_TOKENS
    w_copy = pltpu.make_async_copy(w_hbm, w_ref, w_sem)

    @pl.when(row == 0)
    def _():
        w_copy.start()
        vcat[:, HEAD_SIZE:] = jnp.ones((vcat.shape[0], HEAD_SIZE), vcat.dtype)
        at = 0
        for piece in pieces:
            table[at : at + piece.shape[0]] = piece[...]
            at += piece.shape[0]

    for h in range(heads):
        q4[h * BLOCK_TOKENS : (h + 1) * BLOCK_TOKENS, :] = q_ref[
            :, h * HEAD_SIZE : (h + 1) * HEAD_SIZE
        ]
    for j in range(TOPK):
        rows = slice(j * BLOCK_TOKENS, (j + 1) * BLOCK_TOKENS)
        place = slot[row * TOPK + j]
        kcat[rows, :] = table[place, :, :HEAD_SIZE]
        vcat[rows, :HEAD_SIZE] = table[place, :, HEAD_SIZE:]
    starts = start_ref[...]
    ends = end_ref[...]
    lane = lax.broadcasted_iota(jnp.int32, (BLOCK_TOKENS, BLOCK_TOKENS), 1)
    peak = None
    for c in range(TOPK // CHUNK):
        cols = slice(c * keys, (c + 1) * keys)
        bias = []
        for j in range(c * CHUNK, (c + 1) * CHUNK):
            position = lane + base[row * TOPK + j]
            allowed = (position >= starts) & (position < ends)
            bias.append(jnp.where(allowed, 0.0, negative))
        bias = jnp.concatenate(bias, axis=1)
        raw = lax.dot_general(
            q4[...], kcat[cols, :], (((1,), (1,)), ((), ())), preferred_element_type=jnp.float32
        )
        for h in range(heads):
            rows = slice(h * BLOCK_TOKENS, (h + 1) * BLOCK_TOKENS)
            scores[rows, cols] = raw[rows] * score_scale + bias
        part = scores[:, cols]
        for j in range(CHUNK):
            piece = part[:, j * BLOCK_TOKENS : (j + 1) * BLOCK_TOKENS]
            peak = piece if peak is None else jnp.maximum(peak, piece)
    top = jnp.max(peak, axis=1, keepdims=True)
    total = jnp.zeros((heads * BLOCK_TOKENS, 2 * HEAD_SIZE), jnp.float32)
    for c in range(TOPK // CHUNK):
        cols = slice(c * keys, (c + 1) * keys)
        weights = jnp.exp2(scores[:, cols] - top).astype(jnp.bfloat16)
        total += jnp.dot(weights, vcat[cols, :], preferred_element_type=jnp.float32)
    result = (total[:, :HEAD_SIZE] / total[:, HEAD_SIZE:]).astype(attn.dtype)
    for h in range(heads):
        attn[:, h * HEAD_SIZE : (h + 1) * HEAD_SIZE] = result[
            h * BLOCK_TOKENS : (h + 1) * BLOCK_TOKENS
        ]

    @pl.when(row == 0)
    def _():
        w_copy.wait()

    step = 1024
    for c in range(0, w_ref.shape[1], step):
        out_ref[:, c : c + step] = jnp.dot(
            attn[...], w_ref[:, c : c + step], preferred_element_type=jnp.float32
        ).astype(out_ref.dtype)


def attention(queries, starts, ends, w_out, pieces, slot, base):
    tokens, width = queries.shape
    blocks = tokens // BLOCK_TOKENS
    rows = width // HEAD_SIZE * BLOCK_TOKENS
    listed = TOPK * BLOCK_TOKENS
    per_block = lambda i, *_: (i, 0)
    whole = lambda i, *_: (0, 0, 0)
    table = (sum(p.shape[0] for p in pieces), *pieces[0].shape[1:])
    return pl.pallas_call(
        attention_kernel,
        out_shape=jax.ShapeDtypeStruct((tokens, w_out.shape[1]), jnp.bfloat16),
        grid_spec=pltpu.PrefetchScalarGridSpec(
            num_scalar_prefetch=2,
            grid=(blocks,),
            in_specs=[
                pl.BlockSpec((BLOCK_TOKENS, width), per_block),
                pl.BlockSpec((BLOCK_TOKENS, BLOCK_TOKENS), per_block),
                pl.BlockSpec((BLOCK_TOKENS, BLOCK_TOKENS), per_block),
                pl.BlockSpec(memory_space=pl.ANY),
                *[pl.BlockSpec(piece.shape, whole) for piece in pieces],
            ],
            out_specs=pl.BlockSpec((BLOCK_TOKENS, w_out.shape[1]), per_block),
            scratch_shapes=[
                pltpu.VMEM(table, jnp.bfloat16),
                pltpu.VMEM((rows, HEAD_SIZE), jnp.bfloat16),
                pltpu.VMEM((listed, HEAD_SIZE), jnp.bfloat16),
                pltpu.VMEM((listed, 2 * HEAD_SIZE), jnp.bfloat16),
                pltpu.VMEM((rows, listed), jnp.float32),
                pltpu.VMEM((BLOCK_TOKENS, width), jnp.bfloat16),
                pltpu.VMEM(w_out.shape, w_out.dtype),
                pltpu.SemaphoreType.DMA,
            ],
        ),
        compiler_params=pltpu.CompilerParams(vmem_limit_bytes=44 * 1024 * 1024),
        cost_estimate=pl.CostEstimate(
            flops=4 * blocks * rows * listed * HEAD_SIZE + 2 * tokens * width * w_out.shape[1],
            bytes_accessed=4 * 1024 * 1024,
            transcendentals=blocks * rows * listed,
        ),
        name="attention",
    )(slot, base, queries, starts, ends, w_out, *pieces)


def pick_kernel(piece_count, index, *refs):
    pieces, out_ref = refs[:piece_count], refs[piece_count]
    for r in range(out_ref.shape[0]):
        for d, piece in enumerate(pieces):
            out_ref[r, d] = piece[index[r * piece_count + d]]


def small_kernel(body, out_shape, name, scalars, *operands):
    return pl.pallas_call(
        body,
        out_shape=out_shape,
        in_specs=[pl.BlockSpec(memory_space=pltpu.SMEM)]
        + [pl.BlockSpec(memory_space=pltpu.VMEM)] * len(operands),
        out_specs=jax.tree.map(lambda _: pl.BlockSpec(memory_space=pltpu.VMEM), out_shape),
        compiler_params=pltpu.CompilerParams(vmem_limit_bytes=8 * 1024 * 1024),
        cost_estimate=pl.CostEstimate(
            flops=1024 * 1024, bytes_accessed=1024 * 1024, transcendentals=0
        ),
        name=name,
    )(scalars, *operands)


def pick(pieces, index):
    out = jax.ShapeDtypeStruct((*index.shape, *pieces[0].shape[1:]), pieces[0].dtype)
    body = functools.partial(pick_kernel, len(pieces))
    return small_kernel(body, out, "pick", index.reshape(-1), *pieces)


def shifted(x, axis, shift):
    size = lax.axis_size(axis)
    return lax.ppermute(x, axis, [(i, (i + shift) % size) for i in range(size)])


def ring_gather(x, axis):
    size = lax.axis_size(axis)
    pieces = {0: x}
    for step in range(1, size // 2 + 1):
        pieces[step] = shifted(pieces[step - 1], axis, 1)
        if size - step > step:
            pieces[size - step] = shifted(pieces[(size - step + 1) % size], axis, -1)
    return [pieces[d] for d in range(size)]


def add_kernel(size, groups, me, partial_ref, *refs):
    out_ref = refs[-1]
    arrived = list(refs[:-1])
    at = 0
    for first, rows, distance, terms in groups:
        width = out_ref.shape[1]
        column = pl.multiple_of(lax.rem(me[0] + (distance + size), size) * width, width)
        total = partial_ref[first : first + rows, pl.ds(column, width)].astype(jnp.float32)
        for _ in range(terms):
            total += arrived.pop(0)[...].astype(jnp.float32)
        out_ref[at : at + rows, :] = total.astype(out_ref.dtype)
        at += rows


def ring_scatter(partial, axis, streams):
    size = lax.axis_size(axis)
    me = lax.axis_index(axis).reshape(1).astype(jnp.int32)
    width = partial.shape[1] // size
    rows = partial.shape[0] // streams

    def add(groups, *arrived):
        out = jax.ShapeDtypeStruct((sum(g[1] for g in groups), width), partial.dtype)
        body = functools.partial(add_kernel, size, groups)
        return small_kernel(body, out, "ring_add", me, partial, *arrived)

    far = size // 2
    lengths = [(far, size - 1 - far) if b % 2 == 0 else (size - 1 - far, far) for b in range(streams)]
    sums = [[None, None] for _ in range(streams)]
    for b in range(streams):
        for side, sign in enumerate((1, -1)):
            sums[b][side] = add(((b * rows, rows, sign * lengths[b][side], 0),))
    for step in range(1, far + 1):
        for b in range(streams):
            for side, sign in enumerate((1, -1)):
                left = lengths[b][side] - step
                if left < 0:
                    continue
                moved = shifted(sums[b][side], axis, sign)
                if left:
                    moved = add(((b * rows, rows, sign * left, 1),), moved)
                sums[b][side] = moved
    groups = tuple((b * rows, rows, 0, 2) for b in range(streams))
    return add(groups, *[term for pair in sums for term in pair])


def per_device(y_count, x_count, queries, keys, values, doc_ids, block_lists, w_out):
    tok_rows = queries.shape[0]
    blocks_dev = tok_rows // BLOCK_TOKENS
    seq_count = y_count * x_count
    block_count = blocks_dev * seq_count
    own_y, own_x = lax.axis_index("y"), lax.axis_index("x")
    own_index = own_y * x_count + own_x

    own_blocks = jnp.concatenate([keys, values], axis=1).reshape(
        blocks_dev, BLOCK_TOKENS, 2 * HEAD_SIZE
    )
    column = ring_gather(own_blocks, "y")

    positions = own_index * tok_rows + jnp.arange(tok_rows, dtype=jnp.int32)
    doc_range = jnp.arange(DOCS, dtype=jnp.int32)
    first_local = jnp.min(
        jnp.where(doc_ids[None, :] == doc_range[:, None], positions[None, :], far_position), axis=1
    )
    info = jnp.concatenate([block_lists.reshape(-1), first_local])
    info = lax.all_to_all(
        jnp.broadcast_to(info[None], (seq_count, info.shape[0])), ("y", "x"), 0, 0, tiled=True
    )
    entries = blocks_dev * TOPK
    listing = info[:, :entries]
    firsts = jnp.min(info[:, entries:], axis=0)

    readers = lax.dynamic_slice_in_dim(listing, own_y * x_count, x_count, 0)
    back = jnp.arange(y_count, dtype=jnp.int32)
    owners = (own_y - back + y_count) % y_count * x_count + own_x
    wanted = (readers[:, None, :] < block_count) & (
        readers[:, None, :] // blocks_dev == owners[None, :, None]
    )
    row_offset = jnp.max(jnp.where(wanted, readers[:, None, :] % blocks_dev, 0), axis=2)
    reach = [min(d, y_count - d) for d in range(y_count)]
    near = [d for d in range(y_count) if reach[d] <= y_count // 4]
    far = [d for d in range(y_count) if reach[d] > y_count // 4]
    tables = list(column)
    place = [0] * y_count
    for group in (near, far):
        if not group:
            continue
        first = sum(table.shape[0] for table in tables)
        for at, d in enumerate(group):
            place[d] = (first + at, len(group))
        outgoing = pick([column[d] for d in group], jnp.stack([row_offset[:, d] for d in group], 1))
        arrived = lax.all_to_all(outgoing, "x", 0, 0, tiled=True)
        tables.append(arrived.reshape(-1, *arrived.shape[2:]))

    valid = block_lists < block_count
    owner = block_lists // blocks_dev
    owner_y, owner_x = owner // x_count, owner % x_count
    distance = (own_y - owner_y + y_count) % y_count
    slot = 0
    for d in range(y_count):
        start, stride = place[d]
        slot = jnp.where(distance == d, start + owner_x * stride, slot)
    slot = jnp.where(owner_x == own_x, distance * blocks_dev + block_lists % blocks_dev, slot)
    slot = jnp.where(valid, slot, 0).reshape(-1)
    base = jnp.where(valid, block_lists * BLOCK_TOKENS, null_base).reshape(-1)

    later = doc_range[None, :] > doc_range[:, None]
    ends_doc = jnp.min(jnp.where(later, firsts[None, :], far_position), axis=1)
    match = doc_ids[:, None] == doc_range[None, :]
    starts = jnp.sum(jnp.where(match, firsts[None, :], 0), axis=1)
    ends = jnp.sum(jnp.where(match, ends_doc[None, :], 0), axis=1)
    starts = jnp.broadcast_to(starts[:, None], (tok_rows, BLOCK_TOKENS))
    ends = jnp.broadcast_to(ends[:, None], (tok_rows, BLOCK_TOKENS))

    partial = attention(queries, starts, ends, w_out, tables, slot, base)
    return ring_scatter(partial, "head", 2)


def solution(mesh):
    seq_count = mesh.shape["seq"]
    x_count = 4 if seq_count % 4 == 0 else 1
    y_count = seq_count // x_count
    grid = Mesh(
        mesh.devices.reshape(y_count, x_count, mesh.shape["head"], mesh.shape["dp"]),
        ("y", "x", "head", "dp"),
    )
    rows = ("dp", "y", "x")
    in_specs = (
        P(rows, "head"),
        P(rows, "head"),
        P(rows, "head"),
        P(rows),
        P(rows, None),
        P("head", None),
    )
    return jax.shard_map(
        functools.partial(per_device, y_count, x_count),
        mesh=grid,
        in_specs=in_specs,
        out_specs=P(rows, "head"),
        check_vma=False,
    )
```

```python
import functools
import math

import jax
import jax.numpy as jnp
from jax import lax
from jax.experimental import pallas as pl
from jax.experimental.pallas import tpu as pltpu
from jax.sharding import Mesh, PartitionSpec as P


HEAD_SIZE = 128
BLOCK_TOKENS = 128
DOCS = 8
TOPK = 16
CHUNK = 4

negative = -1e30
far_position = 1073741824
null_base = -1073741824
score_scale = math.log2(math.e) / math.sqrt(HEAD_SIZE)


def attention_kernel(slot, base, start_ref, end_ref, q_hbm, w_hbm, *refs):
    *pieces, out_ref, table, q_all, q4, kcat, vcat, scores, attn, w_ref, sems = refs
    row = pl.program_id(0)
    heads = q_all.shape[1] // HEAD_SIZE
    keys = CHUNK * BLOCK_TOKENS
    w_copy = pltpu.make_async_copy(w_hbm, w_ref, sems.at[0])

    @pl.when(row == 0)
    def _():
        copies = [pltpu.make_async_copy(q_hbm, q_all, sems.at[1])]
        at = 0
        for n, piece in enumerate(pieces):
            place = table.at[at : at + piece.shape[0]]
            copies.append(pltpu.make_async_copy(piece, place, sems.at[n + 2]))
            at += piece.shape[0]
        for copy in copies:
            copy.start()
        w_copy.start()
        vcat[:, HEAD_SIZE:] = jnp.ones((vcat.shape[0], HEAD_SIZE), vcat.dtype)
        for copy in copies:
            copy.wait()

    own = pl.ds(pl.multiple_of(row * BLOCK_TOKENS, BLOCK_TOKENS), BLOCK_TOKENS)
    for h in range(heads):
        q4[h * BLOCK_TOKENS : (h + 1) * BLOCK_TOKENS, :] = q_all[
            own, h * HEAD_SIZE : (h + 1) * HEAD_SIZE
        ]
    for j in range(TOPK):
        rows = slice(j * BLOCK_TOKENS, (j + 1) * BLOCK_TOKENS)
        place = slot[row * TOPK + j]
        kcat[rows, :] = table[place, :, :HEAD_SIZE]
        vcat[rows, :HEAD_SIZE] = table[place, :, HEAD_SIZE:]
    starts = start_ref[...]
    ends = end_ref[...]
    lane = lax.broadcasted_iota(jnp.int32, (BLOCK_TOKENS, BLOCK_TOKENS), 1)
    peak = None
    for c in range(TOPK // CHUNK):
        cols = slice(c * keys, (c + 1) * keys)
        bias = []
        for j in range(c * CHUNK, (c + 1) * CHUNK):
            position = lane + base[row * TOPK + j]
            allowed = (position >= starts) & (position < ends)
            bias.append(jnp.where(allowed, 0.0, negative))
        bias = jnp.concatenate(bias, axis=1)
        raw = lax.dot_general(
            q4[...], kcat[cols, :], (((1,), (1,)), ((), ())), preferred_element_type=jnp.float32
        )
        for h in range(heads):
            rows = slice(h * BLOCK_TOKENS, (h + 1) * BLOCK_TOKENS)
            scores[rows, cols] = raw[rows] * score_scale + bias
        part = scores[:, cols]
        for j in range(CHUNK):
            piece = part[:, j * BLOCK_TOKENS : (j + 1) * BLOCK_TOKENS]
            peak = piece if peak is None else jnp.maximum(peak, piece)
    top = jnp.max(peak, axis=1, keepdims=True)
    total = jnp.zeros((heads * BLOCK_TOKENS, 2 * HEAD_SIZE), jnp.float32)
    for c in range(TOPK // CHUNK):
        cols = slice(c * keys, (c + 1) * keys)
        weights = jnp.exp2(scores[:, cols] - top).astype(jnp.bfloat16)
        total += jnp.dot(weights, vcat[cols, :], preferred_element_type=jnp.float32)
    result = (total[:, :HEAD_SIZE] / total[:, HEAD_SIZE:]).astype(attn.dtype)
    for h in range(heads):
        attn[:, h * HEAD_SIZE : (h + 1) * HEAD_SIZE] = result[
            h * BLOCK_TOKENS : (h + 1) * BLOCK_TOKENS
        ]

    @pl.when(row == 0)
    def _():
        w_copy.wait()

    step = 1024
    for c in range(0, w_ref.shape[1], step):
        out_ref[:, c : c + step] = jnp.dot(
            attn[...], w_ref[:, c : c + step], preferred_element_type=jnp.float32
        ).astype(out_ref.dtype)


def attention(queries, starts, ends, w_out, pieces, slot, base):
    tokens, width = queries.shape
    blocks = tokens // BLOCK_TOKENS
    rows = width // HEAD_SIZE * BLOCK_TOKENS
    listed = TOPK * BLOCK_TOKENS
    per_block = lambda i, *_: (i, 0)
    table = (sum(p.shape[0] for p in pieces), *pieces[0].shape[1:])
    return pl.pallas_call(
        attention_kernel,
        out_shape=jax.ShapeDtypeStruct((tokens, w_out.shape[1]), jnp.bfloat16),
        grid_spec=pltpu.PrefetchScalarGridSpec(
            num_scalar_prefetch=2,
            grid=(blocks,),
            in_specs=[
                pl.BlockSpec((BLOCK_TOKENS, BLOCK_TOKENS), per_block),
                pl.BlockSpec((BLOCK_TOKENS, BLOCK_TOKENS), per_block),
                *[pl.BlockSpec(memory_space=pl.ANY)] * (2 + len(pieces)),
            ],
            out_specs=pl.BlockSpec((BLOCK_TOKENS, w_out.shape[1]), per_block),
            scratch_shapes=[
                pltpu.VMEM(table, jnp.bfloat16),
                pltpu.VMEM(queries.shape, queries.dtype),
                pltpu.VMEM((rows, HEAD_SIZE), jnp.bfloat16),
                pltpu.VMEM((listed, HEAD_SIZE), jnp.bfloat16),
                pltpu.VMEM((listed, 2 * HEAD_SIZE), jnp.bfloat16),
                pltpu.VMEM((rows, listed), jnp.float32),
                pltpu.VMEM((BLOCK_TOKENS, width), jnp.bfloat16),
                pltpu.VMEM(w_out.shape, w_out.dtype),
                pltpu.SemaphoreType.DMA((2 + len(pieces),)),
            ],
        ),
        compiler_params=pltpu.CompilerParams(vmem_limit_bytes=44 * 1024 * 1024),
        cost_estimate=pl.CostEstimate(
            flops=4 * blocks * rows * listed * HEAD_SIZE + 2 * tokens * width * w_out.shape[1],
            bytes_accessed=4 * 1024 * 1024,
            transcendentals=blocks * rows * listed,
        ),
        name="attention",
    )(slot, base, starts, ends, queries, w_out, *pieces)


def pick_kernel(piece_count, index, *refs):
    pieces, out_ref = refs[:piece_count], refs[piece_count]
    for r in range(out_ref.shape[0]):
        for d, piece in enumerate(pieces):
            out_ref[r, d] = piece[index[r * piece_count + d]]


def small_kernel(body, out_shape, scalars, *operands):
    return pl.pallas_call(
        body,
        out_shape=out_shape,
        in_specs=[pl.BlockSpec(memory_space=pltpu.SMEM)]
        + [pl.BlockSpec(memory_space=pltpu.VMEM)] * len(operands),
        out_specs=jax.tree.map(lambda _: pl.BlockSpec(memory_space=pltpu.VMEM), out_shape),
        compiler_params=pltpu.CompilerParams(vmem_limit_bytes=8 * 1024 * 1024),
        cost_estimate=pl.CostEstimate(
            flops=1024 * 1024, bytes_accessed=1024 * 1024, transcendentals=0
        ),
    )(scalars, *operands)


def pick(pieces, index):
    out = jax.ShapeDtypeStruct((*index.shape, *pieces[0].shape[1:]), pieces[0].dtype)
    body = functools.partial(pick_kernel, len(pieces))
    return small_kernel(body, out, index.reshape(-1), *pieces)


def hold_kernel(source_ref, *refs):
    refs[-1][...] = source_ref[...]


def hold(source, *after):
    return pl.pallas_call(
        hold_kernel,
        out_shape=jax.ShapeDtypeStruct(source.shape, source.dtype),
        in_specs=[pl.BlockSpec(memory_space=pltpu.VMEM)]
        + [pl.BlockSpec(memory_space=pl.ANY)] * len(after),
        out_specs=pl.BlockSpec(memory_space=pltpu.VMEM),
        compiler_params=pltpu.CompilerParams(vmem_limit_bytes=1024 * 1024),
        name="hold",
    )(source, *after)


def shifted(x, axis, shift):
    size = lax.axis_size(axis)
    return lax.ppermute(x, axis, [(i, (i + shift) % size) for i in range(size)])


def ring_gather(x, axis):
    size = lax.axis_size(axis)
    pieces = {0: x}
    for step in range(1, size // 2 + 1):
        pieces[step] = shifted(pieces[step - 1], axis, 1)
        if size - step > step:
            pieces[size - step] = shifted(pieces[(size - step + 1) % size], axis, -1)
    return [pieces[d] for d in range(size)]


def add_kernel(size, groups, me, partial_ref, *refs):
    out_ref = refs[-1]
    arrived = list(refs[:-1])
    at = 0
    for first, rows, distance, terms in groups:
        width = out_ref.shape[1]
        column = pl.multiple_of(lax.rem(me[0] + (distance + size), size) * width, width)
        total = partial_ref[first : first + rows, pl.ds(column, width)].astype(jnp.float32)
        for _ in range(terms):
            total += arrived.pop(0)[...].astype(jnp.float32)
        out_ref[at : at + rows, :] = total.astype(out_ref.dtype)
        at += rows


def ring_scatter(partial, axis, streams):
    size = lax.axis_size(axis)
    me = lax.axis_index(axis).reshape(1).astype(jnp.int32)
    width = partial.shape[1] // size
    rows = partial.shape[0] // streams

    def add(groups, *arrived):
        out = jax.ShapeDtypeStruct((sum(g[1] for g in groups), width), partial.dtype)
        body = functools.partial(add_kernel, size, groups)
        return small_kernel(body, out, me, partial, *arrived)

    far = size // 2
    lengths = [(far, size - 1 - far) if b % 2 == 0 else (size - 1 - far, far) for b in range(streams)]
    sums = [[None, None] for _ in range(streams)]
    for b in range(streams):
        for side, sign in enumerate((1, -1)):
            sums[b][side] = add(((b * rows, rows, sign * lengths[b][side], 0),))
    for step in range(1, far + 1):
        for b in range(streams):
            for side, sign in enumerate((1, -1)):
                left = lengths[b][side] - step
                if left < 0:
                    continue
                moved = shifted(sums[b][side], axis, sign)
                if left:
                    moved = add(((b * rows, rows, sign * left, 1),), moved)
                sums[b][side] = moved
    groups = tuple((b * rows, rows, 0, 2) for b in range(streams))
    return add(groups, *[term for pair in sums for term in pair])


def per_device(y_count, x_count, queries, keys, values, doc_ids, block_lists, w_out):
    tok_rows = queries.shape[0]
    blocks_dev = tok_rows // BLOCK_TOKENS
    seq_count = y_count * x_count
    block_count = blocks_dev * seq_count
    own_y, own_x = lax.axis_index("y"), lax.axis_index("x")
    own_index = own_y * x_count + own_x

    own_blocks = jnp.concatenate([keys, values], axis=1).reshape(
        blocks_dev, BLOCK_TOKENS, 2 * HEAD_SIZE
    )
    column = ring_gather(own_blocks, "y")

    positions = own_index * tok_rows + jnp.arange(tok_rows, dtype=jnp.int32)
    doc_range = jnp.arange(DOCS, dtype=jnp.int32)
    first_local = jnp.min(
        jnp.where(doc_ids[None, :] == doc_range[:, None], positions[None, :], far_position), axis=1
    )
    info = jnp.concatenate([block_lists.reshape(-1), first_local])
    info = jnp.broadcast_to(info[None], (seq_count, info.shape[0]))
    info = lax.all_to_all(info, ("y", "x"), 0, 0, tiled=True)
    quarter = y_count // 4
    info = hold(info, column[quarter], column[-quarter])
    entries = blocks_dev * TOPK
    listing = info[:, :entries]
    firsts = jnp.min(info[:, entries:], axis=0)

    readers = lax.dynamic_slice_in_dim(listing, own_y * x_count, x_count, 0)
    back = jnp.arange(y_count, dtype=jnp.int32)
    owners = (own_y - back + y_count) % y_count * x_count + own_x
    wanted = (readers[:, None, :] < block_count) & (
        readers[:, None, :] // blocks_dev == owners[None, :, None]
    )
    row_offset = jnp.max(jnp.where(wanted, readers[:, None, :] % blocks_dev, 0), axis=2)
    reach = [min(d, y_count - d) for d in range(y_count)]
    near = [d for d in range(y_count) if reach[d] <= y_count // 4]
    far = [d for d in range(y_count) if reach[d] > y_count // 4]
    tables = [own_blocks]
    place = [0] * y_count
    for group in (near, far):
        if not group:
            continue
        first = sum(table.shape[0] for table in tables)
        for at, d in enumerate(group):
            place[d] = (first + at, len(group))
        outgoing = pick([column[d] for d in group], jnp.stack([row_offset[:, d] for d in group], 1))
        arrived = lax.all_to_all(outgoing, "x", 0, 0, tiled=True)
        tables.append(arrived.reshape(-1, *arrived.shape[2:]))

    valid = block_lists < block_count
    owner = block_lists // blocks_dev
    owner_y, owner_x = owner // x_count, owner % x_count
    distance = (own_y - owner_y + y_count) % y_count
    slot = 0
    for d in range(y_count):
        start, stride = place[d]
        slot = jnp.where(distance == d, start + owner_x * stride, slot)
    slot = jnp.where(owner == own_index, block_lists % blocks_dev, slot)
    slot = jnp.where(valid, slot, 0).reshape(-1)
    base = jnp.where(valid, block_lists * BLOCK_TOKENS, null_base).reshape(-1)

    later = doc_range[None, :] > doc_range[:, None]
    ends_doc = jnp.min(jnp.where(later, firsts[None, :], far_position), axis=1)
    match = doc_ids[:, None] == doc_range[None, :]
    starts = jnp.sum(jnp.where(match, firsts[None, :], 0), axis=1)
    ends = jnp.sum(jnp.where(match, ends_doc[None, :], 0), axis=1)
    starts = jnp.broadcast_to(starts[:, None], (tok_rows, BLOCK_TOKENS))
    ends = jnp.broadcast_to(ends[:, None], (tok_rows, BLOCK_TOKENS))

    partial = attention(queries, starts, ends, w_out, tables, slot, base)
    return ring_scatter(partial, "head", 2)


def solution(mesh):
    seq_count = mesh.shape["seq"]
    x_count = 4 if seq_count % 4 == 0 else 1
    y_count = seq_count // x_count
    grid = Mesh(
        mesh.devices.reshape(y_count, x_count, mesh.shape["head"], mesh.shape["dp"]),
        ("y", "x", "head", "dp"),
    )
    rows = ("dp", "y", "x")
    in_specs = (
        P(rows, "head"),
        P(rows, "head"),
        P(rows, "head"),
        P(rows),
        P(rows, None),
        P("head", None),
    )

    def body(*operands):
        return per_device(y_count, x_count, *operands)

    return jax.shard_map(
        body, mesh=grid, in_specs=in_specs, out_specs=P(rows, "head"), check_vma=False
    )
```

```python
import functools
import math

import jax
import jax.numpy as jnp
from jax import lax
from jax.experimental import pallas as pl
from jax.experimental.pallas import tpu as pltpu
from jax.sharding import Mesh, PartitionSpec as P


HEAD_SIZE = 128
BLOCK_TOKENS = 128
DOCS = 8
TOPK = 16
CHUNK = 2
SPLIT = 2
WIDTH = 512

negative = -1e30
far_position = 1073741824
null_base = -1073741824
score_scale = math.log2(math.e) / math.sqrt(HEAD_SIZE)


def attention_kernel(slot, base, start_ref, end_ref, q_hbm, w_hbm, *refs):
    *pieces, out_ref, table, q_all, q4, kcat, vcat, scores, attn, w_ref, sems = refs
    row = pl.program_id(0)
    heads = q_all.shape[1] // HEAD_SIZE
    keys = CHUNK * BLOCK_TOKENS
    w_copy = pltpu.make_async_copy(w_hbm, w_ref, sems.at[0])

    @pl.when(row == 0)
    def _():
        copies = [pltpu.make_async_copy(q_hbm, q_all, sems.at[1])]
        at = 0
        for n, piece in enumerate(pieces):
            place = table.at[at : at + piece.shape[0]]
            copies.append(pltpu.make_async_copy(piece, place, sems.at[n + 2]))
            at += piece.shape[0]
        for copy in copies:
            copy.start()
        w_copy.start()
        vcat[:, HEAD_SIZE:] = jnp.ones((vcat.shape[0], HEAD_SIZE), vcat.dtype)
        for copy in copies:
            copy.wait()

    own = pl.ds(pl.multiple_of(row * BLOCK_TOKENS, BLOCK_TOKENS), BLOCK_TOKENS)
    for h in range(heads):
        q4[h * BLOCK_TOKENS : (h + 1) * BLOCK_TOKENS, :] = q_all[
            own, h * HEAD_SIZE : (h + 1) * HEAD_SIZE
        ]
    for j in range(TOPK):
        rows = slice(j * BLOCK_TOKENS, (j + 1) * BLOCK_TOKENS)
        place = slot[row * TOPK + j]
        kcat[rows, :] = table[place, :, :HEAD_SIZE]
        vcat[rows, :HEAD_SIZE] = table[place, :, HEAD_SIZE:]
    starts = start_ref[...]
    ends = end_ref[...]
    lane = lax.broadcasted_iota(jnp.int32, (BLOCK_TOKENS, BLOCK_TOKENS), 1)
    stacked = heads * BLOCK_TOKENS
    peaks = [None] * SPLIT
    for c in range(TOPK // CHUNK):
        cols = slice(c * keys, (c + 1) * keys)
        bias = []
        for j in range(c * CHUNK, (c + 1) * CHUNK):
            position = lane + base[row * TOPK + j]
            allowed = (position >= starts) & (position < ends)
            bias.append(jnp.where(allowed, 0.0, negative))
        for r in range(SPLIT):
            first = r * (stacked // SPLIT)
            raw = lax.dot_general(
                q4[first : first + stacked // SPLIT, :],
                kcat[cols, :],
                (((1,), (1,)), ((), ())),
                preferred_element_type=jnp.float32,
            )
            parts = []
            for h in range(stacked // SPLIT // BLOCK_TOKENS):
                at = slice(h * BLOCK_TOKENS, (h + 1) * BLOCK_TOKENS)
                largest = None
                for j in range(CHUNK):
                    lanes = slice(j * BLOCK_TOKENS, (j + 1) * BLOCK_TOKENS)
                    piece = raw[at, lanes] + bias[j]
                    scores[
                        first + h * BLOCK_TOKENS : first + (h + 1) * BLOCK_TOKENS,
                        (c * CHUNK + j) * BLOCK_TOKENS : (c * CHUNK + j + 1) * BLOCK_TOKENS,
                    ] = piece
                    largest = piece if largest is None else jnp.maximum(largest, piece)
                parts.append(largest)
            largest = jnp.concatenate(parts, axis=0)
            peaks[r] = largest if c == 0 else jnp.maximum(peaks[r], largest)
    tops = [jnp.max(peak, axis=1, keepdims=True) for peak in peaks]
    totals = [jnp.zeros((stacked // SPLIT, 2 * HEAD_SIZE), jnp.float32)] * SPLIT
    for c in range(TOPK // CHUNK):
        cols = slice(c * keys, (c + 1) * keys)
        for r in range(SPLIT):
            at = slice(r * (stacked // SPLIT), (r + 1) * (stacked // SPLIT))
            weights = jnp.exp2((scores[at, cols] - tops[r]) * score_scale).astype(jnp.bfloat16)
            totals[r] += jnp.dot(weights, vcat[cols, :], preferred_element_type=jnp.float32)
    for r in range(SPLIT):
        result = (totals[r][:, :HEAD_SIZE] / totals[r][:, HEAD_SIZE:]).astype(attn.dtype)
        for h in range(heads // SPLIT):
            column = (r * (heads // SPLIT) + h) * HEAD_SIZE
            attn[own, column : column + HEAD_SIZE] = result[
                h * BLOCK_TOKENS : (h + 1) * BLOCK_TOKENS
            ]

    @pl.when(row == pl.num_programs(0) - 1)
    def _():
        w_copy.wait()
        for c in range(0, w_ref.shape[1], WIDTH):
            out_ref[:, c : c + WIDTH] = jnp.dot(
                attn[...], w_ref[:, c : c + WIDTH], preferred_element_type=jnp.float32
            ).astype(out_ref.dtype)


def attention(queries, starts, ends, w_out, pieces, slot, base):
    tokens, width = queries.shape
    blocks = tokens // BLOCK_TOKENS
    rows = width // HEAD_SIZE * BLOCK_TOKENS
    listed = TOPK * BLOCK_TOKENS
    per_block = lambda i, *_: (i, 0)
    table = (sum(p.shape[0] for p in pieces), *pieces[0].shape[1:])
    return pl.pallas_call(
        attention_kernel,
        out_shape=jax.ShapeDtypeStruct((tokens, w_out.shape[1]), jnp.bfloat16),
        grid_spec=pltpu.PrefetchScalarGridSpec(
            num_scalar_prefetch=2,
            grid=(blocks,),
            in_specs=[
                pl.BlockSpec((BLOCK_TOKENS, BLOCK_TOKENS), per_block),
                pl.BlockSpec((BLOCK_TOKENS, BLOCK_TOKENS), per_block),
                *[pl.BlockSpec(memory_space=pl.ANY)] * (2 + len(pieces)),
            ],
            out_specs=pl.BlockSpec(memory_space=pltpu.VMEM),
            scratch_shapes=[
                pltpu.VMEM(table, jnp.bfloat16),
                pltpu.VMEM(queries.shape, queries.dtype),
                pltpu.VMEM((rows, HEAD_SIZE), jnp.bfloat16),
                pltpu.VMEM((listed, HEAD_SIZE), jnp.bfloat16),
                pltpu.VMEM((listed, 2 * HEAD_SIZE), jnp.bfloat16),
                pltpu.VMEM((rows, listed), jnp.float32),
                pltpu.VMEM((tokens, width), jnp.bfloat16),
                pltpu.VMEM(w_out.shape, w_out.dtype),
                pltpu.SemaphoreType.DMA((2 + len(pieces),)),
            ],
        ),
        compiler_params=pltpu.CompilerParams(vmem_limit_bytes=44 * 1024 * 1024),
        cost_estimate=pl.CostEstimate(
            flops=4 * blocks * rows * listed * HEAD_SIZE + 2 * tokens * width * w_out.shape[1],
            bytes_accessed=4 * 1024 * 1024,
            transcendentals=blocks * rows * listed,
        ),
        name="attention",
    )(slot, base, starts, ends, queries, w_out, *pieces)


def pick_kernel(piece_count, index, *refs):
    pieces, out_ref = refs[:piece_count], refs[piece_count]
    for r in range(out_ref.shape[0]):
        for d, piece in enumerate(pieces):
            out_ref[r, d] = piece[index[r * piece_count + d]]


def small_kernel(body, out_shape, scalars, *operands):
    return pl.pallas_call(
        body,
        out_shape=out_shape,
        in_specs=[pl.BlockSpec(memory_space=pltpu.SMEM)]
        + [pl.BlockSpec(memory_space=pltpu.VMEM)] * len(operands),
        out_specs=jax.tree.map(lambda _: pl.BlockSpec(memory_space=pltpu.VMEM), out_shape),
        compiler_params=pltpu.CompilerParams(vmem_limit_bytes=8 * 1024 * 1024),
        cost_estimate=pl.CostEstimate(
            flops=1024 * 1024, bytes_accessed=1024 * 1024, transcendentals=0
        ),
    )(scalars, *operands)


def pick(pieces, index):
    out = jax.ShapeDtypeStruct((*index.shape, *pieces[0].shape[1:]), pieces[0].dtype)
    body = functools.partial(pick_kernel, len(pieces))
    return small_kernel(body, out, index.reshape(-1), *pieces)


def hold_kernel(source_ref, *refs):
    refs[-1][...] = source_ref[...]


def hold(source, *after):
    return pl.pallas_call(
        hold_kernel,
        out_shape=jax.ShapeDtypeStruct(source.shape, source.dtype),
        in_specs=[pl.BlockSpec(memory_space=pltpu.VMEM)]
        + [pl.BlockSpec(memory_space=pl.ANY)] * len(after),
        out_specs=pl.BlockSpec(memory_space=pltpu.VMEM),
        compiler_params=pltpu.CompilerParams(vmem_limit_bytes=1024 * 1024),
        name="hold",
    )(source, *after)


def shifted(x, axis, shift):
    size = lax.axis_size(axis)
    return lax.ppermute(x, axis, [(i, (i + shift) % size) for i in range(size)])


def ring_gather(x, axis):
    size = lax.axis_size(axis)
    pieces = {0: x}
    for step in range(1, size // 2 + 1):
        pieces[step] = shifted(pieces[step - 1], axis, 1)
        if size - step > step:
            pieces[size - step] = shifted(pieces[(size - step + 1) % size], axis, -1)
    return [pieces[d] for d in range(size)]


def add_kernel(size, groups, me, partial_ref, *refs):
    out_ref = refs[-1]
    arrived = list(refs[:-1])
    at = 0
    for first, rows, distance, terms in groups:
        width = out_ref.shape[1]
        column = pl.multiple_of(lax.rem(me[0] + (distance + size), size) * width, width)
        total = partial_ref[first : first + rows, pl.ds(column, width)].astype(jnp.float32)
        for _ in range(terms):
            total += arrived.pop(0)[...].astype(jnp.float32)
        out_ref[at : at + rows, :] = total.astype(out_ref.dtype)
        at += rows


def ring_scatter(partial, axis, streams):
    size = lax.axis_size(axis)
    me = lax.axis_index(axis).reshape(1).astype(jnp.int32)
    width = partial.shape[1] // size
    rows = partial.shape[0] // streams

    def add(groups, *arrived):
        out = jax.ShapeDtypeStruct((sum(g[1] for g in groups), width), partial.dtype)
        body = functools.partial(add_kernel, size, groups)
        return small_kernel(body, out, me, partial, *arrived)

    far = size // 2
    lengths = [(far, size - 1 - far) if b % 2 == 0 else (size - 1 - far, far) for b in range(streams)]
    sums = [[None, None] for _ in range(streams)]
    for b in range(streams):
        for side, sign in enumerate((1, -1)):
            sums[b][side] = add(((b * rows, rows, sign * lengths[b][side], 0),))
    for step in range(1, far + 1):
        for b in range(streams):
            for side, sign in enumerate((1, -1)):
                left = lengths[b][side] - step
                if left < 0:
                    continue
                moved = shifted(sums[b][side], axis, sign)
                if left:
                    moved = add(((b * rows, rows, sign * left, 1),), moved)
                sums[b][side] = moved
    groups = tuple((b * rows, rows, 0, 2) for b in range(streams))
    return add(groups, *[term for pair in sums for term in pair])


def per_device(y_count, x_count, queries, keys, values, doc_ids, block_lists, w_out):
    tok_rows = queries.shape[0]
    blocks_dev = tok_rows // BLOCK_TOKENS
    seq_count = y_count * x_count
    block_count = blocks_dev * seq_count
    own_y, own_x = lax.axis_index("y"), lax.axis_index("x")
    own_index = own_y * x_count + own_x

    own_blocks = jnp.concatenate([keys, values], axis=1).reshape(
        blocks_dev, BLOCK_TOKENS, 2 * HEAD_SIZE
    )
    column = ring_gather(own_blocks, "y")

    positions = own_index * tok_rows + jnp.arange(tok_rows, dtype=jnp.int32)
    doc_range = jnp.arange(DOCS, dtype=jnp.int32)
    first_local = jnp.min(
        jnp.where(doc_ids[None, :] == doc_range[:, None], positions[None, :], far_position), axis=1
    )
    first_local = jnp.pad(first_local, (0, TOPK - DOCS), constant_values=far_position)
    info = jnp.concatenate([block_lists, first_local[None]], axis=0)
    info = jnp.broadcast_to(info[None], (seq_count, *info.shape))
    info = lax.all_to_all(info, ("y", "x"), 0, 0, tiled=True)
    quarter = y_count // 4
    info = hold(info, column[quarter], column[-quarter])
    listing = info[:, :blocks_dev]
    firsts = jnp.min(info[:, blocks_dev, :DOCS], axis=0)

    readers = lax.dynamic_slice_in_dim(listing, own_y * x_count, x_count, 0)
    back = jnp.arange(y_count, dtype=jnp.int32)
    owners = (own_y - back + y_count) % y_count * x_count + own_x
    readers = readers[:, None]
    wanted = (readers < block_count) & (readers // blocks_dev == owners[None, :, None, None])
    row_offset = jnp.max(jnp.where(wanted, readers % blocks_dev, 0), axis=(2, 3))
    reach = [min(d, y_count - d) for d in range(y_count)]
    near = [d for d in range(y_count) if reach[d] <= y_count // 4]
    far = [d for d in range(y_count) if reach[d] > y_count // 4]
    tables = [own_blocks]
    place = [0] * y_count
    for group in (near, far):
        if not group:
            continue
        first = sum(table.shape[0] for table in tables)
        for at, d in enumerate(group):
            place[d] = (first + at, len(group))
        outgoing = pick([column[d] for d in group], jnp.stack([row_offset[:, d] for d in group], 1))
        arrived = lax.all_to_all(outgoing, "x", 0, 0, tiled=True)
        tables.append(arrived.reshape(-1, *arrived.shape[2:]))

    valid = block_lists < block_count
    owner = block_lists // blocks_dev
    owner_y, owner_x = owner // x_count, owner % x_count
    distance = (own_y - owner_y + y_count) % y_count
    slot = 0
    for d in range(y_count):
        start, stride = place[d]
        slot = jnp.where(distance == d, start + owner_x * stride, slot)
    slot = jnp.where(owner == own_index, block_lists % blocks_dev, slot)
    slot = jnp.where(valid, slot, 0).reshape(-1)
    base = jnp.where(valid, block_lists * BLOCK_TOKENS, null_base).reshape(-1)

    later = doc_range[None, :] > doc_range[:, None]
    ends_doc = jnp.min(jnp.where(later, firsts[None, :], far_position), axis=1)
    match = doc_ids[:, None] == doc_range[None, :]
    starts = jnp.sum(jnp.where(match, firsts[None, :], 0), axis=1)
    ends = jnp.sum(jnp.where(match, ends_doc[None, :], 0), axis=1)
    starts = jnp.broadcast_to(starts[:, None], (tok_rows, BLOCK_TOKENS))
    ends = jnp.broadcast_to(ends[:, None], (tok_rows, BLOCK_TOKENS))

    partial = attention(queries, starts, ends, w_out, tables, slot, base)
    return ring_scatter(partial, "head", 2)


def solution(mesh):
    seq_count = mesh.shape["seq"]
    x_count = 4 if seq_count % 4 == 0 else 1
    y_count = seq_count // x_count
    grid = Mesh(
        mesh.devices.reshape(y_count, x_count, mesh.shape["head"], mesh.shape["dp"]),
        ("y", "x", "head", "dp"),
    )
    rows = ("dp", "y", "x")
    in_specs = (
        P(rows, "head"),
        P(rows, "head"),
        P(rows, "head"),
        P(rows),
        P(rows, None),
        P("head", None),
    )

    def body(*operands):
        return per_device(y_count, x_count, *operands)

    return jax.shard_map(
        body, mesh=grid, in_specs=in_specs, out_specs=P(rows, "head"), check_vma=False
    )
```

```python
import functools
import math

import jax
import jax.numpy as jnp
from jax import lax
from jax.experimental import pallas as pl
from jax.experimental.pallas import tpu as pltpu
from jax.sharding import Mesh, PartitionSpec as P


HEAD_SIZE = 128
BLOCK_TOKENS = 128
DOCS = 8
TOPK = 16
CHUNK = 2
SPLIT = 2
WIDTH = 512

negative = -1e30
far_position = 1073741824
null_base = -1073741824
score_scale = math.log2(math.e) / math.sqrt(HEAD_SIZE)


def attention_kernel(slot, base, start_ref, end_ref, q_hbm, w_hbm, *refs):
    *pieces, out_ref, table, q_all, q4, kcat, vcat, scores, attn, w_ref, sems = refs
    row = pl.program_id(0)
    heads = q_all.shape[1] // HEAD_SIZE
    keys = CHUNK * BLOCK_TOKENS
    w_copy = pltpu.make_async_copy(w_hbm, w_ref, sems.at[0])

    @pl.when(row == 0)
    def _():
        copies = [pltpu.make_async_copy(q_hbm, q_all, sems.at[1])]
        at = 0
        for n, piece in enumerate(pieces):
            place = table.at[at : at + piece.shape[0]]
            copies.append(pltpu.make_async_copy(piece, place, sems.at[n + 2]))
            at += piece.shape[0]
        for copy in copies:
            copy.start()
        w_copy.start()
        vcat[:, HEAD_SIZE:] = jnp.ones((vcat.shape[0], HEAD_SIZE), vcat.dtype)
        for copy in copies:
            copy.wait()

    own = pl.ds(pl.multiple_of(row * BLOCK_TOKENS, BLOCK_TOKENS), BLOCK_TOKENS)
    for h in range(heads):
        q4[h * BLOCK_TOKENS : (h + 1) * BLOCK_TOKENS, :] = q_all[
            own, h * HEAD_SIZE : (h + 1) * HEAD_SIZE
        ]
    for j in range(TOPK):
        rows = slice(j * BLOCK_TOKENS, (j + 1) * BLOCK_TOKENS)
        place = slot[row * TOPK + j]
        kcat[rows, :] = table[place, :, :HEAD_SIZE]
        vcat[rows, :HEAD_SIZE] = table[place, :, HEAD_SIZE:]
    starts = start_ref[...]
    ends = end_ref[...]
    lane = lax.broadcasted_iota(jnp.int32, (BLOCK_TOKENS, BLOCK_TOKENS), 1)
    stacked = heads * BLOCK_TOKENS
    peaks = [None] * SPLIT
    for c in range(TOPK // CHUNK):
        cols = slice(c * keys, (c + 1) * keys)
        bias = []
        for j in range(c * CHUNK, (c + 1) * CHUNK):
            position = lane + base[row * TOPK + j]
            allowed = (position >= starts) & (position < ends)
            bias.append(jnp.where(allowed, 0.0, negative))
        for r in range(SPLIT):
            first = r * (stacked // SPLIT)
            raw = lax.dot_general(
                q4[first : first + stacked // SPLIT, :],
                kcat[cols, :],
                (((1,), (1,)), ((), ())),
                preferred_element_type=jnp.float32,
            )
            parts = []
            for h in range(stacked // SPLIT // BLOCK_TOKENS):
                at = slice(h * BLOCK_TOKENS, (h + 1) * BLOCK_TOKENS)
                largest = None
                for j in range(CHUNK):
                    lanes = slice(j * BLOCK_TOKENS, (j + 1) * BLOCK_TOKENS)
                    piece = raw[at, lanes] + bias[j]
                    scores[
                        first + h * BLOCK_TOKENS : first + (h + 1) * BLOCK_TOKENS,
                        (c * CHUNK + j) * BLOCK_TOKENS : (c * CHUNK + j + 1) * BLOCK_TOKENS,
                    ] = piece
                    largest = piece if largest is None else jnp.maximum(largest, piece)
                parts.append(largest)
            largest = jnp.concatenate(parts, axis=0)
            peaks[r] = largest if c == 0 else jnp.maximum(peaks[r], largest)
    tops = [jnp.max(peak, axis=1, keepdims=True) for peak in peaks]
    totals = [jnp.zeros((stacked // SPLIT, 2 * HEAD_SIZE), jnp.float32)] * SPLIT
    for c in range(TOPK // CHUNK):
        cols = slice(c * keys, (c + 1) * keys)
        for r in range(SPLIT):
            at = slice(r * (stacked // SPLIT), (r + 1) * (stacked // SPLIT))
            weights = jnp.exp2((scores[at, cols] - tops[r]) * score_scale).astype(jnp.bfloat16)
            totals[r] += jnp.dot(weights, vcat[cols, :], preferred_element_type=jnp.float32)
    for r in range(SPLIT):
        result = (totals[r][:, :HEAD_SIZE] / totals[r][:, HEAD_SIZE:]).astype(attn.dtype)
        for h in range(heads // SPLIT):
            column = (r * (heads // SPLIT) + h) * HEAD_SIZE
            attn[own, column : column + HEAD_SIZE] = result[
                h * BLOCK_TOKENS : (h + 1) * BLOCK_TOKENS
            ]

    @pl.when(row == pl.num_programs(0) - 1)
    def _():
        w_copy.wait()
        for c in range(0, w_ref.shape[1], WIDTH):
            out_ref[:, c : c + WIDTH] = jnp.dot(
                attn[...], w_ref[:, c : c + WIDTH], preferred_element_type=jnp.float32
            ).astype(out_ref.dtype)


def attention(queries, starts, ends, w_out, pieces, slot, base):
    tokens, width = queries.shape
    blocks = tokens // BLOCK_TOKENS
    rows = width // HEAD_SIZE * BLOCK_TOKENS
    listed = TOPK * BLOCK_TOKENS
    per_block = lambda i, *_: (i, 0)
    table = (sum(p.shape[0] for p in pieces), *pieces[0].shape[1:])
    return pl.pallas_call(
        attention_kernel,
        out_shape=jax.ShapeDtypeStruct((tokens, w_out.shape[1]), jnp.bfloat16),
        grid_spec=pltpu.PrefetchScalarGridSpec(
            num_scalar_prefetch=2,
            grid=(blocks,),
            in_specs=[
                pl.BlockSpec((BLOCK_TOKENS, BLOCK_TOKENS), per_block),
                pl.BlockSpec((BLOCK_TOKENS, BLOCK_TOKENS), per_block),
                *[pl.BlockSpec(memory_space=pl.ANY)] * (2 + len(pieces)),
            ],
            out_specs=pl.BlockSpec(memory_space=pltpu.VMEM),
            scratch_shapes=[
                pltpu.VMEM(table, jnp.bfloat16),
                pltpu.VMEM(queries.shape, queries.dtype),
                pltpu.VMEM((rows, HEAD_SIZE), jnp.bfloat16),
                pltpu.VMEM((listed, HEAD_SIZE), jnp.bfloat16),
                pltpu.VMEM((listed, 2 * HEAD_SIZE), jnp.bfloat16),
                pltpu.VMEM((rows, listed), jnp.float32),
                pltpu.VMEM((tokens, width), jnp.bfloat16),
                pltpu.VMEM(w_out.shape, w_out.dtype),
                pltpu.SemaphoreType.DMA((2 + len(pieces),)),
            ],
        ),
        compiler_params=pltpu.CompilerParams(vmem_limit_bytes=44 * 1024 * 1024),
        cost_estimate=pl.CostEstimate(
            flops=4 * blocks * rows * listed * HEAD_SIZE + 2 * tokens * width * w_out.shape[1],
            bytes_accessed=4 * 1024 * 1024,
            transcendentals=blocks * rows * listed,
        ),
        name="attention",
    )(slot, base, starts, ends, queries, w_out, *pieces)


def pick_kernel(piece_count, index, *refs):
    pieces, out_ref, sems = refs[:piece_count], refs[piece_count], refs[piece_count + 1]
    copies = [
        pltpu.make_async_copy(
            piece.at[index[r * piece_count + d]],
            out_ref.at[r, d],
            sems.at[r * piece_count + d],
        )
        for r in range(out_ref.shape[0])
        for d, piece in enumerate(pieces)
    ]
    for copy in copies:
        copy.start()
    for copy in copies:
        copy.wait()


def info_kernel(tok_rows, me, docs_ref, lists_ref, out_ref):
    docs = docs_ref[...]
    shape = docs.shape
    positions = (
        me[0] * tok_rows
        + lax.broadcasted_iota(jnp.int32, shape, 0) * shape[1]
        + lax.broadcasted_iota(jnp.int32, shape, 1)
    )
    lane = lax.broadcasted_iota(jnp.int32, (1, TOPK), 1)
    firsts = jnp.full((1, TOPK), far_position, jnp.int32)
    for d in range(DOCS):
        first = jnp.min(jnp.where(docs == d, positions, far_position))
        firsts = jnp.where(lane == d, first, firsts)
    rows = lists_ref.shape[0]
    for r in range(out_ref.shape[0]):
        out_ref[r, :rows, :] = lists_ref[...]
        out_ref[r, rows:, :] = firsts


def small_kernel(body, out_shape, scalars, *operands, mib=8):
    return pl.pallas_call(
        body,
        out_shape=out_shape,
        in_specs=[pl.BlockSpec(memory_space=pltpu.SMEM)]
        + [pl.BlockSpec(memory_space=pltpu.VMEM)] * len(operands),
        out_specs=jax.tree.map(lambda _: pl.BlockSpec(memory_space=pltpu.VMEM), out_shape),
        compiler_params=pltpu.CompilerParams(vmem_limit_bytes=mib and mib * 1024 * 1024),
        cost_estimate=pl.CostEstimate(
            flops=1024 * 1024, bytes_accessed=1024 * 1024, transcendentals=0
        ),
    )(scalars, *operands)


def pick(pieces, index):
    return pl.pallas_call(
        functools.partial(pick_kernel, len(pieces)),
        out_shape=jax.ShapeDtypeStruct((*index.shape, *pieces[0].shape[1:]), pieces[0].dtype),
        in_specs=[pl.BlockSpec(memory_space=pltpu.SMEM)]
        + [pl.BlockSpec(memory_space=pl.ANY)] * len(pieces),
        out_specs=pl.BlockSpec(memory_space=pl.ANY),
        scratch_shapes=[pltpu.SemaphoreType.DMA((index.size,))],
        compiler_params=pltpu.CompilerParams(vmem_limit_bytes=1024 * 1024),
        cost_estimate=pl.CostEstimate(
            flops=1024 * 1024, bytes_accessed=1024 * 1024, transcendentals=0
        ),
        name="pick",
    )(index.reshape(-1), *pieces)


def hold_kernel(source_ref, *refs):
    refs[-1][...] = source_ref[...]


def hold(source, *after):
    return pl.pallas_call(
        hold_kernel,
        out_shape=jax.ShapeDtypeStruct(source.shape, source.dtype),
        in_specs=[pl.BlockSpec(memory_space=pltpu.VMEM)]
        + [pl.BlockSpec(memory_space=pl.ANY)] * len(after),
        out_specs=pl.BlockSpec(memory_space=pltpu.VMEM),
        compiler_params=pltpu.CompilerParams(vmem_limit_bytes=1024 * 1024),
        name="hold",
    )(source, *after)


def shifted(x, axis, shift):
    size = lax.axis_size(axis)
    return lax.ppermute(x, axis, [(i, (i + shift) % size) for i in range(size)])


def ring_gather(x, axis):
    size = lax.axis_size(axis)
    pieces = {0: x}
    for step in range(1, size // 2 + 1):
        pieces[step] = shifted(pieces[step - 1], axis, 1)
        if size - step > step:
            pieces[size - step] = shifted(pieces[(size - step + 1) % size], axis, -1)
    return [pieces[d] for d in range(size)]


def add_kernel(size, groups, me, partial_ref, *refs):
    out_ref = refs[-1]
    arrived = list(refs[:-1])
    at = 0
    for first, rows, distance, terms in groups:
        width = out_ref.shape[1]
        column = pl.multiple_of(lax.rem(me[0] + (distance + size), size) * width, width)
        total = partial_ref[first : first + rows, pl.ds(column, width)].astype(jnp.float32)
        for _ in range(terms):
            total += arrived.pop(0)[...].astype(jnp.float32)
        out_ref[at : at + rows, :] = total.astype(out_ref.dtype)
        at += rows


def ring_scatter(partial, axis, streams):
    size = lax.axis_size(axis)
    me = lax.axis_index(axis).reshape(1).astype(jnp.int32)
    width = partial.shape[1] // size
    rows = partial.shape[0] // streams

    def add(groups, *arrived):
        out = jax.ShapeDtypeStruct((sum(g[1] for g in groups), width), partial.dtype)
        body = functools.partial(add_kernel, size, groups)
        return small_kernel(body, out, me, partial, *arrived)

    far = size // 2
    lengths = [(far, size - 1 - far) if b % 2 == 0 else (size - 1 - far, far) for b in range(streams)]
    sums = [[None, None] for _ in range(streams)]
    for b in range(streams):
        for side, sign in enumerate((1, -1)):
            sums[b][side] = add(((b * rows, rows, sign * lengths[b][side], 0),))
    for step in range(1, far + 1):
        for b in range(streams):
            for side, sign in enumerate((1, -1)):
                left = lengths[b][side] - step
                if left < 0:
                    continue
                moved = shifted(sums[b][side], axis, sign)
                if left:
                    moved = add(((b * rows, rows, sign * left, 1),), moved)
                sums[b][side] = moved
    groups = tuple((b * rows, rows, 0, 2) for b in range(streams))
    return add(groups, *[term for pair in sums for term in pair])


def per_device(y_count, x_count, queries, keys, values, doc_ids, block_lists, w_out):
    tok_rows = queries.shape[0]
    blocks_dev = tok_rows // BLOCK_TOKENS
    seq_count = y_count * x_count
    block_count = blocks_dev * seq_count
    own_y, own_x = lax.axis_index("y"), lax.axis_index("x")
    own_index = own_y * x_count + own_x

    own_blocks = jnp.concatenate([keys, values], axis=1).reshape(
        blocks_dev, BLOCK_TOKENS, 2 * HEAD_SIZE
    )
    column = ring_gather(own_blocks, "y")

    doc_range = jnp.arange(DOCS, dtype=jnp.int32)
    info = small_kernel(
        functools.partial(info_kernel, tok_rows),
        jax.ShapeDtypeStruct((seq_count, blocks_dev + 1, TOPK), jnp.int32),
        own_index.reshape(1).astype(jnp.int32),
        doc_ids.reshape(blocks_dev, BLOCK_TOKENS),
        block_lists,
        mib=None,
    )
    info = lax.all_to_all(info, ("y", "x"), 0, 0, tiled=True)
    quarter = y_count // 4
    info = hold(info, column[quarter], column[-quarter])
    listing = info[:, :blocks_dev]
    firsts = jnp.min(info[:, blocks_dev, :DOCS], axis=0)

    readers = lax.dynamic_slice_in_dim(listing, own_y * x_count, x_count, 0)
    back = jnp.arange(y_count, dtype=jnp.int32)
    owners = (own_y - back + y_count) % y_count * x_count + own_x
    readers = readers[:, None]
    wanted = (readers < block_count) & (readers // blocks_dev == owners[None, :, None, None])
    row_offset = jnp.max(jnp.where(wanted, readers % blocks_dev, 0), axis=(2, 3))
    reach = [min(d, y_count - d) for d in range(y_count)]
    near = [d for d in range(y_count) if reach[d] <= y_count // 4]
    far = [d for d in range(y_count) if reach[d] > y_count // 4]
    tables = [own_blocks]
    place = [0] * y_count
    for group in (near, far):
        if not group:
            continue
        first = sum(table.shape[0] for table in tables)
        for at, d in enumerate(group):
            place[d] = (first + at, len(group))
        outgoing = pick([column[d] for d in group], jnp.stack([row_offset[:, d] for d in group], 1))
        arrived = lax.all_to_all(outgoing, "x", 0, 0, tiled=True)
        tables.append(arrived.reshape(-1, *arrived.shape[2:]))

    valid = block_lists < block_count
    owner = block_lists // blocks_dev
    owner_y, owner_x = owner // x_count, owner % x_count
    distance = (own_y - owner_y + y_count) % y_count
    slot = 0
    for d in range(y_count):
        start, stride = place[d]
        slot = jnp.where(distance == d, start + owner_x * stride, slot)
    slot = jnp.where(owner == own_index, block_lists % blocks_dev, slot)
    slot = jnp.where(valid, slot, 0).reshape(-1)
    base = jnp.where(valid, block_lists * BLOCK_TOKENS, null_base).reshape(-1)

    later = doc_range[None, :] > doc_range[:, None]
    ends_doc = jnp.min(jnp.where(later, firsts[None, :], far_position), axis=1)
    match = doc_ids[:, None] == doc_range[None, :]
    starts = jnp.sum(jnp.where(match, firsts[None, :], 0), axis=1)
    ends = jnp.sum(jnp.where(match, ends_doc[None, :], 0), axis=1)
    starts = jnp.broadcast_to(starts[:, None], (tok_rows, BLOCK_TOKENS))
    ends = jnp.broadcast_to(ends[:, None], (tok_rows, BLOCK_TOKENS))

    partial = attention(queries, starts, ends, w_out, tables, slot, base)
    return ring_scatter(partial, "head", 2)


def solution(mesh):
    seq_count = mesh.shape["seq"]
    x_count = 4 if seq_count % 4 == 0 else 1
    y_count = seq_count // x_count
    grid = Mesh(
        mesh.devices.reshape(y_count, x_count, mesh.shape["head"], mesh.shape["dp"]),
        ("y", "x", "head", "dp"),
    )
    rows = ("dp", "y", "x")
    in_specs = (
        P(rows, "head"),
        P(rows, "head"),
        P(rows, "head"),
        P(rows),
        P(rows, None),
        P("head", None),
    )

    def body(*operands):
        return per_device(y_count, x_count, *operands)

    return jax.shard_map(
        body, mesh=grid, in_specs=in_specs, out_specs=P(rows, "head"), check_vma=False
    )
```

```python
import functools
import math

import jax
import jax.numpy as jnp
from jax import lax
from jax.experimental import pallas as pl
from jax.experimental.pallas import tpu as pltpu
from jax.sharding import Mesh, PartitionSpec as P


HEAD_SIZE = 128
BLOCK_TOKENS = 128
DOCS = 8
TOPK = 16
CHUNK = 2
SPLIT = 2
WIDTH = 512

negative = -1e30
far_position = 1073741824
null_base = -1073741824
score_scale = math.log2(math.e) / math.sqrt(HEAD_SIZE)


def attention_kernel(slot, base, start_ref, end_ref, q_hbm, w_hbm, *refs):
    *pieces, out_ref, table, q_all, q4, kcat, vcat, scores, attn, w_ref, sems = refs
    row = pl.program_id(0)
    heads = q_all.shape[1] // HEAD_SIZE
    keys = CHUNK * BLOCK_TOKENS
    w_copy = pltpu.make_async_copy(w_hbm, w_ref, sems.at[0])

    @pl.when(row == 0)
    def _():
        copies = [pltpu.make_async_copy(q_hbm, q_all, sems.at[1])]
        at = 0
        for n, piece in enumerate(pieces):
            place = table.at[at : at + piece.shape[0]]
            copies.append(pltpu.make_async_copy(piece, place, sems.at[n + 2]))
            at += piece.shape[0]
        for copy in copies:
            copy.start()
        w_copy.start()
        vcat[:, HEAD_SIZE:] = jnp.ones((vcat.shape[0], HEAD_SIZE), vcat.dtype)
        for copy in copies:
            copy.wait()

    own = pl.ds(pl.multiple_of(row * BLOCK_TOKENS, BLOCK_TOKENS), BLOCK_TOKENS)
    for h in range(heads):
        q4[h * BLOCK_TOKENS : (h + 1) * BLOCK_TOKENS, :] = q_all[
            own, h * HEAD_SIZE : (h + 1) * HEAD_SIZE
        ]
    for j in range(TOPK):
        rows = slice(j * BLOCK_TOKENS, (j + 1) * BLOCK_TOKENS)
        place = slot[row * TOPK + j]
        kcat[rows, :] = table[place, :, :HEAD_SIZE]
        vcat[rows, :HEAD_SIZE] = table[place, :, HEAD_SIZE:]
    starts = start_ref[...]
    ends = end_ref[...]
    lane = lax.broadcasted_iota(jnp.int32, (BLOCK_TOKENS, BLOCK_TOKENS), 1)
    stacked = heads * BLOCK_TOKENS
    peaks = [None] * SPLIT
    for c in range(TOPK // CHUNK):
        cols = slice(c * keys, (c + 1) * keys)
        bias = []
        for j in range(c * CHUNK, (c + 1) * CHUNK):
            position = lane + base[row * TOPK + j]
            allowed = (position >= starts) & (position < ends)
            bias.append(jnp.where(allowed, 0.0, negative))
        for r in range(SPLIT):
            first = r * (stacked // SPLIT)
            raw = lax.dot_general(
                q4[first : first + stacked // SPLIT, :],
                kcat[cols, :],
                (((1,), (1,)), ((), ())),
                preferred_element_type=jnp.float32,
            )
            parts = []
            for h in range(stacked // SPLIT // BLOCK_TOKENS):
                at = slice(h * BLOCK_TOKENS, (h + 1) * BLOCK_TOKENS)
                largest = None
                for j in range(CHUNK):
                    lanes = slice(j * BLOCK_TOKENS, (j + 1) * BLOCK_TOKENS)
                    piece = raw[at, lanes] + bias[j]
                    scores[
                        first + h * BLOCK_TOKENS : first + (h + 1) * BLOCK_TOKENS,
                        (c * CHUNK + j) * BLOCK_TOKENS : (c * CHUNK + j + 1) * BLOCK_TOKENS,
                    ] = piece
                    largest = piece if largest is None else jnp.maximum(largest, piece)
                parts.append(largest)
            largest = jnp.concatenate(parts, axis=0)
            peaks[r] = largest if c == 0 else jnp.maximum(peaks[r], largest)
    tops = [jnp.max(peak, axis=1, keepdims=True) for peak in peaks]
    totals = [jnp.zeros((stacked // SPLIT, 2 * HEAD_SIZE), jnp.float32)] * SPLIT
    for c in range(TOPK // CHUNK):
        cols = slice(c * keys, (c + 1) * keys)
        for r in range(SPLIT):
            at = slice(r * (stacked // SPLIT), (r + 1) * (stacked // SPLIT))
            weights = jnp.exp2((scores[at, cols] - tops[r]) * score_scale).astype(jnp.bfloat16)
            totals[r] += jnp.dot(weights, vcat[cols, :], preferred_element_type=jnp.float32)
    for r in range(SPLIT):
        result = (totals[r][:, :HEAD_SIZE] / totals[r][:, HEAD_SIZE:]).astype(attn.dtype)
        for h in range(heads // SPLIT):
            column = (r * (heads // SPLIT) + h) * HEAD_SIZE
            attn[own, column : column + HEAD_SIZE] = result[
                h * BLOCK_TOKENS : (h + 1) * BLOCK_TOKENS
            ]

    @pl.when(row == pl.num_programs(0) - 1)
    def _():
        w_copy.wait()
        for c in range(0, w_ref.shape[1], WIDTH):
            out_ref[:, c : c + WIDTH] = jnp.dot(
                attn[...], w_ref[:, c : c + WIDTH], preferred_element_type=jnp.float32
            ).astype(out_ref.dtype)


def attention(queries, starts, ends, w_out, pieces, slot, base):
    tokens, width = queries.shape
    blocks = tokens // BLOCK_TOKENS
    rows = width // HEAD_SIZE * BLOCK_TOKENS
    listed = TOPK * BLOCK_TOKENS
    per_block = lambda i, *_: (i, 0)
    table = (sum(p.shape[0] for p in pieces), *pieces[0].shape[1:])
    return pl.pallas_call(
        attention_kernel,
        out_shape=jax.ShapeDtypeStruct((tokens, w_out.shape[1]), jnp.bfloat16),
        grid_spec=pltpu.PrefetchScalarGridSpec(
            num_scalar_prefetch=2,
            grid=(blocks,),
            in_specs=[
                pl.BlockSpec((BLOCK_TOKENS, BLOCK_TOKENS), per_block),
                pl.BlockSpec((BLOCK_TOKENS, BLOCK_TOKENS), per_block),
                *[pl.BlockSpec(memory_space=pl.ANY)] * (2 + len(pieces)),
            ],
            out_specs=pl.BlockSpec(memory_space=pltpu.VMEM),
            scratch_shapes=[
                pltpu.VMEM(table, jnp.bfloat16),
                pltpu.VMEM(queries.shape, queries.dtype),
                pltpu.VMEM((rows, HEAD_SIZE), jnp.bfloat16),
                pltpu.VMEM((listed, HEAD_SIZE), jnp.bfloat16),
                pltpu.VMEM((listed, 2 * HEAD_SIZE), jnp.bfloat16),
                pltpu.VMEM((rows, listed), jnp.float32),
                pltpu.VMEM((tokens, width), jnp.bfloat16),
                pltpu.VMEM(w_out.shape, w_out.dtype),
                pltpu.SemaphoreType.DMA((2 + len(pieces),)),
            ],
        ),
        compiler_params=pltpu.CompilerParams(vmem_limit_bytes=44 * 1024 * 1024),
        cost_estimate=pl.CostEstimate(
            flops=4 * blocks * rows * listed * HEAD_SIZE + 2 * tokens * width * w_out.shape[1],
            bytes_accessed=4 * 1024 * 1024,
            transcendentals=blocks * rows * listed,
        ),
        name="attention",
    )(slot, base, starts, ends, queries, w_out, *pieces)


def pick_kernel(piece_count, index, *refs):
    pieces, out_ref, sems = refs[:piece_count], refs[piece_count], refs[piece_count + 1]
    copies = [
        pltpu.make_async_copy(
            piece.at[index[r * piece_count + d]],
            out_ref.at[r, d],
            sems.at[r * piece_count + d],
        )
        for r in range(out_ref.shape[0])
        for d, piece in enumerate(pieces)
    ]
    for copy in copies:
        copy.start()
    for copy in copies:
        copy.wait()


def info_kernel(tok_rows, me, docs_ref, lists_ref, out_ref):
    docs = docs_ref[...]
    shape = docs.shape
    positions = (
        me[0] * tok_rows
        + lax.broadcasted_iota(jnp.int32, shape, 0) * shape[1]
        + lax.broadcasted_iota(jnp.int32, shape, 1)
    )
    lane = lax.broadcasted_iota(jnp.int32, (1, TOPK), 1)
    firsts = jnp.full((1, TOPK), far_position, jnp.int32)
    for d in range(DOCS):
        first = jnp.min(jnp.where(docs == d, positions, far_position))
        firsts = jnp.where(lane == d, first, firsts)
    rows = lists_ref.shape[0]
    for r in range(out_ref.shape[0]):
        out_ref[r, :rows, :] = lists_ref[...]
        out_ref[r, rows:, :] = firsts


def small_kernel(body, out_shape, scalars, *operands, mib=8):
    return pl.pallas_call(
        body,
        out_shape=out_shape,
        in_specs=[pl.BlockSpec(memory_space=pltpu.SMEM)]
        + [pl.BlockSpec(memory_space=pltpu.VMEM)] * len(operands),
        out_specs=jax.tree.map(lambda _: pl.BlockSpec(memory_space=pltpu.VMEM), out_shape),
        compiler_params=pltpu.CompilerParams(vmem_limit_bytes=mib and mib * 1024 * 1024),
        cost_estimate=pl.CostEstimate(
            flops=1024 * 1024, bytes_accessed=1024 * 1024, transcendentals=0
        ),
    )(scalars, *operands)


def pick(pieces, index):
    return pl.pallas_call(
        functools.partial(pick_kernel, len(pieces)),
        out_shape=jax.ShapeDtypeStruct((*index.shape, *pieces[0].shape[1:]), pieces[0].dtype),
        in_specs=[pl.BlockSpec(memory_space=pltpu.SMEM)]
        + [pl.BlockSpec(memory_space=pl.ANY)] * len(pieces),
        out_specs=pl.BlockSpec(memory_space=pl.ANY),
        scratch_shapes=[pltpu.SemaphoreType.DMA((index.size,))],
        compiler_params=pltpu.CompilerParams(vmem_limit_bytes=1024 * 1024),
        cost_estimate=pl.CostEstimate(
            flops=1024 * 1024, bytes_accessed=1024 * 1024, transcendentals=0
        ),
        name="pick",
    )(index.reshape(-1), *pieces)


def hold_kernel(source_ref, *refs):
    refs[-1][...] = source_ref[...]


def hold(source, *after):
    return pl.pallas_call(
        hold_kernel,
        out_shape=jax.ShapeDtypeStruct(source.shape, source.dtype),
        in_specs=[pl.BlockSpec(memory_space=pltpu.VMEM)]
        + [pl.BlockSpec(memory_space=pl.ANY)] * len(after),
        out_specs=pl.BlockSpec(memory_space=pltpu.VMEM),
        compiler_params=pltpu.CompilerParams(vmem_limit_bytes=1024 * 1024),
        name="hold",
    )(source, *after)


def shifted(x, axis, shift):
    size = lax.axis_size(axis)
    return lax.ppermute(x, axis, [(i, (i + shift) % size) for i in range(size)])


def ring_gather(x, axis):
    size = lax.axis_size(axis)
    pieces = {0: x}
    for step in range(1, size // 2 + 1):
        pieces[step] = shifted(pieces[step - 1], axis, 1)
        if size - step > step:
            pieces[size - step] = shifted(pieces[(size - step + 1) % size], axis, -1)
    return [pieces[d] for d in range(size)]


def add_kernel(size, groups, me, partial_ref, *refs):
    out_ref = refs[-1]
    arrived = list(refs[:-1])
    at = 0
    for first, rows, distance, terms in groups:
        width = out_ref.shape[1]
        column = pl.multiple_of(lax.rem(me[0] + (distance + size), size) * width, width)
        total = partial_ref[first : first + rows, pl.ds(column, width)].astype(jnp.float32)
        for _ in range(terms):
            total += arrived.pop(0)[...].astype(jnp.float32)
        out_ref[at : at + rows, :] = total.astype(out_ref.dtype)
        at += rows


def ring_scatter(partial, axis):
    size = lax.axis_size(axis)
    me = lax.axis_index(axis).reshape(1).astype(jnp.int32)
    width = partial.shape[1] // size
    tokens = partial.shape[0]
    split = tokens * 5 // 8 if tokens % 128 == 0 else tokens // 2
    parts = ((0, split), (split, tokens - split))
    streams = len(parts)

    def add(groups, *arrived):
        out = jax.ShapeDtypeStruct((sum(g[1] for g in groups), width), partial.dtype)
        body = functools.partial(add_kernel, size, groups)
        return small_kernel(body, out, me, partial, *arrived)

    far = size // 2
    lengths = [(far, size - 1 - far) if b % 2 == 0 else (size - 1 - far, far) for b in range(streams)]
    moved = [[None, None] for _ in range(streams)]
    for step in range(far):
        for b in range(streams):
            for side, sign in enumerate((1, -1)):
                left = lengths[b][side] - step
                if left <= 0:
                    continue
                arrived = [moved[b][side]] if step else []
                running = add(((*parts[b], sign * left, len(arrived)),), *arrived)
                moved[b][side] = shifted(running, axis, sign)
    groups = tuple((*part, 0, 2) for part in parts)
    return add(groups, *[term for pair in moved for term in pair])


def per_device(y_count, x_count, queries, keys, values, doc_ids, block_lists, w_out):
    tok_rows = queries.shape[0]
    blocks_dev = tok_rows // BLOCK_TOKENS
    seq_count = y_count * x_count
    block_count = blocks_dev * seq_count
    own_y, own_x = lax.axis_index("y"), lax.axis_index("x")
    own_index = own_y * x_count + own_x

    own_blocks = jnp.concatenate([keys, values], axis=1).reshape(
        blocks_dev, BLOCK_TOKENS, 2 * HEAD_SIZE
    )
    column = ring_gather(own_blocks, "y")

    doc_range = jnp.arange(DOCS, dtype=jnp.int32)
    info = small_kernel(
        functools.partial(info_kernel, tok_rows),
        jax.ShapeDtypeStruct((seq_count, blocks_dev + 1, TOPK), jnp.int32),
        own_index.reshape(1).astype(jnp.int32),
        doc_ids.reshape(blocks_dev, BLOCK_TOKENS),
        block_lists,
        mib=None,
    )
    info = lax.all_to_all(info, ("y", "x"), 0, 0, tiled=True)
    quarter = y_count // 4
    info = hold(info, column[quarter], column[-quarter])
    listing = info[:, :blocks_dev]
    firsts = jnp.min(info[:, blocks_dev, :DOCS], axis=0)

    readers = lax.dynamic_slice_in_dim(listing, own_y * x_count, x_count, 0)
    back = jnp.arange(y_count, dtype=jnp.int32)
    owners = (own_y - back + y_count) % y_count * x_count + own_x
    readers = readers[:, None]
    wanted = (readers < block_count) & (readers // blocks_dev == owners[None, :, None, None])
    row_offset = jnp.max(jnp.where(wanted, readers % blocks_dev, 0), axis=(2, 3))
    reach = [min(d, y_count - d) for d in range(y_count)]
    near = [d for d in range(y_count) if reach[d] <= y_count // 4]
    far = [d for d in range(y_count) if reach[d] > y_count // 4]
    tables = [own_blocks]
    place = [0] * y_count
    for group in (near, far):
        if not group:
            continue
        first = sum(table.shape[0] for table in tables)
        for at, d in enumerate(group):
            place[d] = (first + at, len(group))
        outgoing = pick([column[d] for d in group], jnp.stack([row_offset[:, d] for d in group], 1))
        arrived = lax.all_to_all(outgoing, "x", 0, 0, tiled=True)
        tables.append(arrived.reshape(-1, *arrived.shape[2:]))

    valid = block_lists < block_count
    owner = block_lists // blocks_dev
    owner_y, owner_x = owner // x_count, owner % x_count
    distance = (own_y - owner_y + y_count) % y_count
    slot = 0
    for d in range(y_count):
        start, stride = place[d]
        slot = jnp.where(distance == d, start + owner_x * stride, slot)
    slot = jnp.where(owner == own_index, block_lists % blocks_dev, slot)
    slot = jnp.where(valid, slot, 0).reshape(-1)
    base = jnp.where(valid, block_lists * BLOCK_TOKENS, null_base).reshape(-1)

    later = doc_range[None, :] > doc_range[:, None]
    ends_doc = jnp.min(jnp.where(later, firsts[None, :], far_position), axis=1)
    match = doc_ids[:, None] == doc_range[None, :]
    starts = jnp.sum(jnp.where(match, firsts[None, :], 0), axis=1)
    ends = jnp.sum(jnp.where(match, ends_doc[None, :], 0), axis=1)
    starts = jnp.broadcast_to(starts[:, None], (tok_rows, BLOCK_TOKENS))
    ends = jnp.broadcast_to(ends[:, None], (tok_rows, BLOCK_TOKENS))

    partial = attention(queries, starts, ends, w_out, tables, slot, base)
    return ring_scatter(partial, "head")


def solution(mesh):
    seq_count = mesh.shape["seq"]
    x_count = 4 if seq_count % 4 == 0 else 1
    y_count = seq_count // x_count
    grid = Mesh(
        mesh.devices.reshape(y_count, x_count, mesh.shape["head"], mesh.shape["dp"]),
        ("y", "x", "head", "dp"),
    )
    rows = ("dp", "y", "x")
    in_specs = (
        P(rows, "head"),
        P(rows, "head"),
        P(rows, "head"),
        P(rows),
        P(rows, None),
        P("head", None),
    )

    def body(*operands):
        return per_device(y_count, x_count, *operands)

    return jax.shard_map(
        body, mesh=grid, in_specs=in_specs, out_specs=P(rows, "head"), check_vma=False
    )
```

```python
import functools
import math

import jax
import jax.numpy as jnp
from jax import lax
from jax.experimental import pallas as pl
from jax.experimental.pallas import tpu as pltpu
from jax.sharding import Mesh, PartitionSpec as P


HEAD_SIZE = 128
BLOCK_TOKENS = 128
DOCS = 8
TOPK = 16
CHUNK = 2
SPLIT = 2
WIDTH = 512

negative = -1e30
far_position = 1073741824
null_base = -1073741824
score_scale = math.log2(math.e) / math.sqrt(HEAD_SIZE)


def attention_kernel(slot, base, start_ref, end_ref, q_hbm, w_hbm, *refs):
    *pieces, out_ref, table, q_all, q4, kcat, vcat, scores, attn, w_ref, sems = refs
    row = pl.program_id(0)
    heads = q_all.shape[1] // HEAD_SIZE
    keys = CHUNK * BLOCK_TOKENS
    w_copy = pltpu.make_async_copy(w_hbm, w_ref, sems.at[0])

    @pl.when(row == 0)
    def _():
        copies = [pltpu.make_async_copy(q_hbm, q_all, sems.at[1])]
        at = 0
        for n, piece in enumerate(pieces):
            place = table.at[at : at + piece.shape[0]]
            copies.append(pltpu.make_async_copy(piece, place, sems.at[n + 2]))
            at += piece.shape[0]
        for copy in copies:
            copy.start()
        w_copy.start()
        vcat[:, HEAD_SIZE:] = jnp.ones((vcat.shape[0], HEAD_SIZE), vcat.dtype)
        for copy in copies:
            copy.wait()

    own = pl.ds(pl.multiple_of(row * BLOCK_TOKENS, BLOCK_TOKENS), BLOCK_TOKENS)
    for h in range(heads):
        q4[h * BLOCK_TOKENS : (h + 1) * BLOCK_TOKENS, :] = q_all[
            own, h * HEAD_SIZE : (h + 1) * HEAD_SIZE
        ]
    for j in range(TOPK):
        rows = slice(j * BLOCK_TOKENS, (j + 1) * BLOCK_TOKENS)
        place = slot[row * TOPK + j]
        kcat[rows, :] = table[place, :, :HEAD_SIZE]
        vcat[rows, :HEAD_SIZE] = table[place, :, HEAD_SIZE:]
    starts = start_ref[...]
    ends = end_ref[...]
    lane = lax.broadcasted_iota(jnp.int32, (BLOCK_TOKENS, BLOCK_TOKENS), 1)
    stacked = heads * BLOCK_TOKENS
    peaks = [None] * SPLIT
    for c in range(TOPK // CHUNK):
        cols = slice(c * keys, (c + 1) * keys)
        bias = []
        for j in range(c * CHUNK, (c + 1) * CHUNK):
            position = lane + base[row * TOPK + j]
            allowed = (position >= starts) & (position < ends)
            bias.append(jnp.where(allowed, 0.0, negative))
        for r in range(SPLIT):
            first = r * (stacked // SPLIT)
            raw = lax.dot_general(
                q4[first : first + stacked // SPLIT, :],
                kcat[cols, :],
                (((1,), (1,)), ((), ())),
                preferred_element_type=jnp.float32,
            )
            parts = []
            for h in range(stacked // SPLIT // BLOCK_TOKENS):
                at = slice(h * BLOCK_TOKENS, (h + 1) * BLOCK_TOKENS)
                largest = None
                for j in range(CHUNK):
                    lanes = slice(j * BLOCK_TOKENS, (j + 1) * BLOCK_TOKENS)
                    piece = raw[at, lanes] + bias[j]
                    scores[
                        first + h * BLOCK_TOKENS : first + (h + 1) * BLOCK_TOKENS,
                        (c * CHUNK + j) * BLOCK_TOKENS : (c * CHUNK + j + 1) * BLOCK_TOKENS,
                    ] = piece
                    largest = piece if largest is None else jnp.maximum(largest, piece)
                parts.append(largest)
            largest = jnp.concatenate(parts, axis=0)
            peaks[r] = largest if c == 0 else jnp.maximum(peaks[r], largest)
    tops = [jnp.max(peak, axis=1, keepdims=True) for peak in peaks]
    totals = [jnp.zeros((stacked // SPLIT, 2 * HEAD_SIZE), jnp.float32)] * SPLIT
    for c in range(TOPK // CHUNK):
        cols = slice(c * keys, (c + 1) * keys)
        for r in range(SPLIT):
            at = slice(r * (stacked // SPLIT), (r + 1) * (stacked // SPLIT))
            weights = jnp.exp2((scores[at, cols] - tops[r]) * score_scale).astype(jnp.bfloat16)
            totals[r] += jnp.dot(weights, vcat[cols, :], preferred_element_type=jnp.float32)
    for r in range(SPLIT):
        result = (totals[r][:, :HEAD_SIZE] / totals[r][:, HEAD_SIZE:]).astype(attn.dtype)
        for h in range(heads // SPLIT):
            column = (r * (heads // SPLIT) + h) * HEAD_SIZE
            attn[own, column : column + HEAD_SIZE] = result[
                h * BLOCK_TOKENS : (h + 1) * BLOCK_TOKENS
            ]

    @pl.when(row == pl.num_programs(0) - 1)
    def _():
        w_copy.wait()
        for c in range(0, w_ref.shape[1], WIDTH):
            out_ref[:, c : c + WIDTH] = jnp.dot(
                attn[...], w_ref[:, c : c + WIDTH], preferred_element_type=jnp.float32
            ).astype(out_ref.dtype)


def attention(queries, starts, ends, w_out, pieces, slot, base):
    tokens, width = queries.shape
    blocks = tokens // BLOCK_TOKENS
    rows = width // HEAD_SIZE * BLOCK_TOKENS
    listed = TOPK * BLOCK_TOKENS
    per_block = lambda i, *_: (i, 0)
    table = (sum(p.shape[0] for p in pieces), *pieces[0].shape[1:])
    return pl.pallas_call(
        attention_kernel,
        out_shape=jax.ShapeDtypeStruct((tokens, w_out.shape[1]), jnp.bfloat16),
        grid_spec=pltpu.PrefetchScalarGridSpec(
            num_scalar_prefetch=2,
            grid=(blocks,),
            in_specs=[
                pl.BlockSpec((BLOCK_TOKENS, BLOCK_TOKENS), per_block),
                pl.BlockSpec((BLOCK_TOKENS, BLOCK_TOKENS), per_block),
                *[pl.BlockSpec(memory_space=pl.ANY)] * (2 + len(pieces)),
            ],
            out_specs=pl.BlockSpec(memory_space=pltpu.VMEM),
            scratch_shapes=[
                pltpu.VMEM(table, jnp.bfloat16),
                pltpu.VMEM(queries.shape, queries.dtype),
                pltpu.VMEM((rows, HEAD_SIZE), jnp.bfloat16),
                pltpu.VMEM((listed, HEAD_SIZE), jnp.bfloat16),
                pltpu.VMEM((listed, 2 * HEAD_SIZE), jnp.bfloat16),
                pltpu.VMEM((rows, listed), jnp.float32),
                pltpu.VMEM((tokens, width), jnp.bfloat16),
                pltpu.VMEM(w_out.shape, w_out.dtype),
                pltpu.SemaphoreType.DMA((2 + len(pieces),)),
            ],
        ),
        compiler_params=pltpu.CompilerParams(vmem_limit_bytes=44 * 1024 * 1024),
        cost_estimate=pl.CostEstimate(
            flops=4 * blocks * rows * listed * HEAD_SIZE + 2 * tokens * width * w_out.shape[1],
            bytes_accessed=4 * 1024 * 1024,
            transcendentals=blocks * rows * listed,
        ),
        name="attention",
    )(slot, base, starts, ends, queries, w_out, *pieces)


def pick_kernel(piece_count, index, *refs):
    pieces, out_ref, sems = refs[:piece_count], refs[piece_count], refs[piece_count + 1]
    copies = [
        pltpu.make_async_copy(
            piece.at[index[r * piece_count + d]],
            out_ref.at[r, d],
            sems.at[r * piece_count + d],
        )
        for r in range(out_ref.shape[0])
        for d, piece in enumerate(pieces)
    ]
    for copy in copies:
        copy.start()
    for copy in copies:
        copy.wait()


def info_kernel(tok_rows, me, docs_ref, lists_ref, out_ref):
    docs = docs_ref[...]
    shape = docs.shape
    positions = (
        me[0] * tok_rows
        + lax.broadcasted_iota(jnp.int32, shape, 0) * shape[1]
        + lax.broadcasted_iota(jnp.int32, shape, 1)
    )
    lane = lax.broadcasted_iota(jnp.int32, (1, TOPK), 1)
    firsts = jnp.full((1, TOPK), far_position, jnp.int32)
    for d in range(DOCS):
        first = jnp.min(jnp.where(docs == d, positions, far_position))
        firsts = jnp.where(lane == d, first, firsts)
    rows = lists_ref.shape[0]
    for r in range(out_ref.shape[0]):
        out_ref[r, :rows, :] = lists_ref[...]
        out_ref[r, rows:, :] = firsts


def small_kernel(body, out_shape, scalars, *operands, mib=8):
    return pl.pallas_call(
        body,
        out_shape=out_shape,
        in_specs=[pl.BlockSpec(memory_space=pltpu.SMEM)]
        + [pl.BlockSpec(memory_space=pltpu.VMEM)] * len(operands),
        out_specs=jax.tree.map(lambda _: pl.BlockSpec(memory_space=pltpu.VMEM), out_shape),
        compiler_params=pltpu.CompilerParams(vmem_limit_bytes=mib and mib * 1024 * 1024),
        cost_estimate=pl.CostEstimate(
            flops=1024 * 1024, bytes_accessed=1024 * 1024, transcendentals=0
        ),
    )(scalars, *operands)


def pick(pieces, index):
    return pl.pallas_call(
        functools.partial(pick_kernel, len(pieces)),
        out_shape=jax.ShapeDtypeStruct((*index.shape, *pieces[0].shape[1:]), pieces[0].dtype),
        in_specs=[pl.BlockSpec(memory_space=pltpu.SMEM)]
        + [pl.BlockSpec(memory_space=pl.ANY)] * len(pieces),
        out_specs=pl.BlockSpec(memory_space=pl.ANY),
        scratch_shapes=[pltpu.SemaphoreType.DMA((index.size,))],
        compiler_params=pltpu.CompilerParams(vmem_limit_bytes=1024 * 1024),
        cost_estimate=pl.CostEstimate(
            flops=1024 * 1024, bytes_accessed=1024 * 1024, transcendentals=0
        ),
        name="pick",
    )(index.reshape(-1), *pieces)


def hold_kernel(source_ref, *refs):
    refs[-1][...] = source_ref[...]


def hold(source, *after):
    return pl.pallas_call(
        hold_kernel,
        out_shape=jax.ShapeDtypeStruct(source.shape, source.dtype),
        in_specs=[pl.BlockSpec(memory_space=pltpu.VMEM)]
        + [pl.BlockSpec(memory_space=pl.ANY)] * len(after),
        out_specs=pl.BlockSpec(memory_space=pltpu.VMEM),
        compiler_params=pltpu.CompilerParams(vmem_limit_bytes=1024 * 1024),
        name="hold",
    )(source, *after)


def shifted(x, axis, shift):
    size = lax.axis_size(axis)
    return lax.ppermute(x, axis, [(i, (i + shift) % size) for i in range(size)])


def ring_gather(x, axis):
    size = lax.axis_size(axis)
    pieces = {0: x}
    for step in range(1, size // 2 + 1):
        pieces[step] = shifted(pieces[step - 1], axis, 1)
        if size - step > step:
            pieces[size - step] = shifted(pieces[(size - step + 1) % size], axis, -1)
    return [pieces[d] for d in range(size)]


def add_kernel(size, groups, me, partial_ref, *refs):
    out_ref = refs[-1]
    arrived = list(refs[:-1])
    at = 0
    for first, rows, distance, terms in groups:
        width = out_ref.shape[1]
        column = pl.multiple_of(lax.rem(me[0] + (distance + size), size) * width, width)
        total = partial_ref[first : first + rows, pl.ds(column, width)].astype(jnp.float32)
        for _ in range(terms):
            total += arrived.pop(0)[...].astype(jnp.float32)
        out_ref[at : at + rows, :] = total.astype(out_ref.dtype)
        at += rows


def ring_scatter(partial, axis):
    size = lax.axis_size(axis)
    me = lax.axis_index(axis).reshape(1).astype(jnp.int32)
    width = partial.shape[1] // size
    tokens = partial.shape[0]
    split = tokens * 21 // 32 if tokens % 256 == 0 else tokens // 2
    parts = ((0, split), (split, tokens - split))
    streams = len(parts)

    def add(groups, *arrived):
        out = jax.ShapeDtypeStruct((sum(g[1] for g in groups), width), partial.dtype)
        body = functools.partial(add_kernel, size, groups)
        return small_kernel(body, out, me, partial, *arrived)

    far = size // 2
    lengths = [(far, size - 1 - far) if b % 2 == 0 else (size - 1 - far, far) for b in range(streams)]
    moved = [[None, None] for _ in range(streams)]
    for step in range(far):
        for b, side in ((0, 0), (1, 1), (0, 1), (1, 0)):
            sign = (1, -1)[side]
            left = lengths[b][side] - step
            if left <= 0:
                continue
            arrived = [moved[b][side]] if step else []
            running = add(((*parts[b], sign * left, len(arrived)),), *arrived)
            moved[b][side] = shifted(running, axis, sign)
    groups = tuple((*part, 0, 2) for part in parts)
    return add(groups, *[term for pair in moved for term in pair])


def per_device(y_count, x_count, queries, keys, values, doc_ids, block_lists, w_out):
    tok_rows = queries.shape[0]
    blocks_dev = tok_rows // BLOCK_TOKENS
    seq_count = y_count * x_count
    block_count = blocks_dev * seq_count
    own_y, own_x = lax.axis_index("y"), lax.axis_index("x")
    own_index = own_y * x_count + own_x

    own_blocks = jnp.concatenate([keys, values], axis=1).reshape(
        blocks_dev, BLOCK_TOKENS, 2 * HEAD_SIZE
    )
    column = ring_gather(own_blocks, "y")

    doc_range = jnp.arange(DOCS, dtype=jnp.int32)
    info = small_kernel(
        functools.partial(info_kernel, tok_rows),
        jax.ShapeDtypeStruct((seq_count, blocks_dev + 1, TOPK), jnp.int32),
        own_index.reshape(1).astype(jnp.int32),
        doc_ids.reshape(blocks_dev, BLOCK_TOKENS),
        block_lists,
        mib=None,
    )
    info = lax.all_to_all(info, ("y", "x"), 0, 0, tiled=True)
    quarter = y_count // 4
    info = hold(info, column[quarter], column[-quarter])
    listing = info[:, :blocks_dev]
    firsts = jnp.min(info[:, blocks_dev, :DOCS], axis=0)

    readers = lax.dynamic_slice_in_dim(listing, own_y * x_count, x_count, 0)
    back = jnp.arange(y_count, dtype=jnp.int32)
    owners = (own_y - back + y_count) % y_count * x_count + own_x
    readers = readers[:, None]
    wanted = (readers < block_count) & (readers // blocks_dev == owners[None, :, None, None])
    row_offset = jnp.max(jnp.where(wanted, readers % blocks_dev, 0), axis=(2, 3))
    reach = [min(d, y_count - d) for d in range(y_count)]
    near = [d for d in range(y_count) if reach[d] <= y_count // 4]
    far = [d for d in range(y_count) if reach[d] > y_count // 4]
    tables = [own_blocks]
    place = [0] * y_count
    for group in (near, far):
        if not group:
            continue
        first = sum(table.shape[0] for table in tables)
        for at, d in enumerate(group):
            place[d] = (first + at, len(group))
        outgoing = pick([column[d] for d in group], jnp.stack([row_offset[:, d] for d in group], 1))
        arrived = lax.all_to_all(outgoing, "x", 0, 0, tiled=True)
        tables.append(arrived.reshape(-1, *arrived.shape[2:]))

    valid = block_lists < block_count
    owner = block_lists // blocks_dev
    owner_y, owner_x = owner // x_count, owner % x_count
    distance = (own_y - owner_y + y_count) % y_count
    slot = 0
    for d in range(y_count):
        start, stride = place[d]
        slot = jnp.where(distance == d, start + owner_x * stride, slot)
    slot = jnp.where(owner == own_index, block_lists % blocks_dev, slot)
    slot = jnp.where(valid, slot, 0).reshape(-1)
    base = jnp.where(valid, block_lists * BLOCK_TOKENS, null_base).reshape(-1)

    later = doc_range[None, :] > doc_range[:, None]
    ends_doc = jnp.min(jnp.where(later, firsts[None, :], far_position), axis=1)
    match = doc_ids[:, None] == doc_range[None, :]
    starts = jnp.sum(jnp.where(match, firsts[None, :], 0), axis=1)
    ends = jnp.sum(jnp.where(match, ends_doc[None, :], 0), axis=1)
    starts = jnp.broadcast_to(starts[:, None], (tok_rows, BLOCK_TOKENS))
    ends = jnp.broadcast_to(ends[:, None], (tok_rows, BLOCK_TOKENS))

    partial = attention(queries, starts, ends, w_out, tables, slot, base)
    return ring_scatter(partial, "head")


def solution(mesh):
    seq_count = mesh.shape["seq"]
    x_count = 4 if seq_count % 4 == 0 else 1
    y_count = seq_count // x_count
    grid = Mesh(
        mesh.devices.reshape(y_count, x_count, mesh.shape["head"], mesh.shape["dp"]),
        ("y", "x", "head", "dp"),
    )
    rows = ("dp", "y", "x")
    in_specs = (
        P(rows, "head"),
        P(rows, "head"),
        P(rows, "head"),
        P(rows),
        P(rows, None),
        P("head", None),
    )

    def body(*operands):
        return per_device(y_count, x_count, *operands)

    return jax.shard_map(
        body, mesh=grid, in_specs=in_specs, out_specs=P(rows, "head"), check_vma=False
    )
```
